32 devices in a mesh: members: 2 (over x), zonal: 8 (over z, y), merid: 2 (over core).
Axes of the slice: x: 2, y: 2, z: 4, core: 2. Of those that a mesh axis runs over, the one named last changes fastest.
Arguments:
- height: float32 [256, 1024], P(('members', 'zonal'), 'merid'), parts along dimension 0, may hold values from -6 to 6
- transport_u: float32 [256, 1024], P(('members', 'zonal'), 'merid'), parts along dimension 0, may hold values from -4 to 4
- transport_v: float32 [256, 1024], P(('members', 'zonal'), 'merid'), parts along dimension 0, may hold values from -4 to 4
- thickness: float32 [14, 256, 1024], P(None, ('members', 'zonal'), 'merid'), parts along dimension 1, may hold values from 0.5 to 2
- velocity_u: float32 [14, 256, 1024], P(None, ('members', 'zonal'), 'merid'), parts along dimension 1, may hold values from -3 to 3
- velocity_v: float32 [14, 256, 1024], P(None, ('members', 'zonal'), 'merid'), parts along dimension 1, may hold values from -3 to 3
- sea_faces: int32 [2, 128, 1024], P(None, 'zonal', 'merid'), may hold values 0 or 1
- wind_seeds: int32 [8, 2], P('members'), parts along dimension 0, may hold values from 1 to 96
- wind_scale: float32 [8], P('members'), parts along dimension 0, may hold values from 0.5 to 2
- wind_base: float32 [2, 128, 1024], P(None, 'zonal', 'merid'), may hold values from -6 to 6
Outputs:
- final_height: float32 [256, 1024], P(('members', 'zonal'), 'merid'), parts along dimension 0
- final_transport_u: float32 [256, 1024], P(('members', 'zonal'), 'merid'), parts along dimension 0
- final_transport_v: float32 [256, 1024], P(('members', 'zonal'), 'merid'), parts along dimension 0
- final_thickness: float32 [14, 256, 1024], P(None, ('members', 'zonal'), 'merid'), parts along dimension 1
- final_velocity_u: float32 [14, 256, 1024], P(None, ('members', 'zonal'), 'merid'), parts along dimension 1
- final_velocity_v: float32 [14, 256, 1024], P(None, ('members', 'zonal'), 'merid'), parts along dimension 1
The draws below stay inside these ranges and needn't reach their ends.
There are 2 independent parts, one for each index of `members`. The reference program is written for one: setup_inputs(seed, part) draws one part's arguments, and reference() takes and returns one part's arrays. A program takes and returns all parts, laid end to end along the dimension named above; an argument that names none is the same for every part. Nothing has to cross between parts.
All inputs are finite; a program needn't handle non-finite values. No bound on the sum of `sea_faces` on one device may be relied on, other than what follows from the above.
Results may differ from the reference program's by a relative error of at most 0.0001.
Values sent between devices are 32-bit elements; how exact they have to be, the bound alone decides.
A program may use at most 64 MiB of HBM per device.

```python
import math
import jax
import jax.numpy as jnp

LAYERS = 14
NSUB = 6
STEPS = 2
MODES = 4
NX = 128
NY = 1024


def plant(result, stream_key, least, top_value):
    spot = [jax.random.randint(jax.random.fold_in(stream_key, axis), (), 0, length) for axis, length in enumerate(result.shape)]
    widest = result.shape.index(max(result.shape))
    beside = spot[:widest] + [(spot[widest] + 1) % result.shape[widest]] + spot[widest + 1:]
    return result.at[tuple(spot)].set(least).at[tuple(beside)].set(top_value)


def block_scale(own_key, extent, shards, least, largest):
    def one(dim, blocks):
        heights = jax.random.uniform(jax.random.fold_in(jax.random.fold_in(own_key, 6), dim), (blocks,), jnp.float32, least / len(shards), largest / len(shards))
        return jnp.repeat(jnp.exp(heights), extent[dim] // blocks).reshape((-1,) + (1,) * (len(extent) - dim - 1))

    gain = one(*shards[0])
    for cut in shards[1:]:
        gain = gain * one(*cut)
    return gain


def noise(rng, shape, deviation, limit, split=(), kind=jnp.bfloat16):
    gain = block_scale(rng, shape, split, -0.22, 0.18) if split else 1.0
    entries = jax.random.normal(rng, shape, jnp.float32) * deviation * gain
    return jnp.minimum(jnp.maximum(entries, -limit), limit).astype(kind)


def setup_inputs(seed: int = 0, part: int = 0) -> dict:
    splits = jax.random.split(jax.random.key(seed), 11)
    part_splits = jax.random.split(jax.random.fold_in(splits[10], part), 11)
    return {
        "height": noise(part_splits[0], (NX, NY), 1.0, 6.0, ((0, 8), (1, 2)), jnp.float32),
        "transport_u": noise(part_splits[1], (NX, NY), 0.5, 4.0, ((0, 8), (1, 2)), jnp.float32),
        "transport_v": noise(part_splits[2], (NX, NY), 0.5, 4.0, ((0, 8), (1, 2)), jnp.float32),
        "thickness": jnp.clip(jnp.exp(math.log(2.0) - 1.3862944 * jax.random.uniform(part_splits[3], (LAYERS, NX, NY), jnp.float32) ** block_scale(part_splits[3], (LAYERS, NX, NY), ((1, 8), (2, 2)), -0.2, 0.2)), 0.5, 2.0),
        "velocity_u": noise(part_splits[4], (LAYERS, NX, NY), 0.5, 3.0, ((1, 8), (2, 2)), jnp.float32),
        "velocity_v": noise(part_splits[5], (LAYERS, NX, NY), 0.5, 3.0, ((1, 8), (2, 2)), jnp.float32),
        "sea_faces": plant((jax.random.randint(splits[6], (2, NX, NY), 0, 8) < 7).astype(jnp.int32), jax.random.fold_in(splits[6], 1), 0, 1),
        "wind_seeds": plant(jax.random.randint(part_splits[7], (MODES, 2), 1, 97), jax.random.fold_in(part_splits[7], 1), 1, 96).astype(jnp.int32),
        "wind_scale": jnp.clip(jnp.exp(jax.random.uniform(part_splits[8], (MODES,), jnp.float32, math.log(0.5), math.log(2.0))), 0.5, 2.0),
        "wind_base": noise(splits[9], (2, NX, NY), 1.0, 6.0, ((1, 8), (2, 2)), jnp.float32),
    }


WAVE_LIMIT = 0.225
STRESS_SCALE = 0.1
FLUX_STEP = 0.05
PRESS_COEF = 0.05


def east(field):
    return jnp.roll(field, -1, axis=-2)


def west(field):
    return jnp.roll(field, 1, axis=-2)


def north(field):
    folded = jnp.flip(field[..., -1], axis=-1)
    return jnp.concatenate([field[..., 1:], folded[..., None]], axis=-1)


def south(field):
    return jnp.concatenate([jnp.zeros_like(field[..., :1]), field[..., :-1]], axis=-1)


def reference(height, transport_u, transport_v, thickness, velocity_u, velocity_v, sea_faces, wind_seeds, wind_scale, wind_base):
    total_x = height.shape[0]
    total_y = height.shape[1]
    mask_u = sea_faces[0].astype(jnp.float32)
    mask_v = sea_faces[1].astype(jnp.float32)
    columns = jnp.arange(total_x, dtype=jnp.int32)
    rows_idx = jnp.arange(total_y, dtype=jnp.int32)
    wave_x = wind_seeds[:, 0].astype(jnp.int32)
    wave_y = wind_seeds[:, 1].astype(jnp.int32)
    phase = ((wave_x[:, None, None] * columns[None, :, None]) % total_x).astype(jnp.float32) / total_x
    phase = phase + ((wave_y[:, None, None] * rows_idx[None, None, :]) % total_y).astype(jnp.float32) / total_y
    angle = (2.0 * math.pi) * phase
    amplitude = wind_scale[:, None, None]
    stress_x = STRESS_SCALE * (wind_base[0] + jnp.sum(amplitude * jnp.cos(angle), axis=0))
    stress_y = STRESS_SCALE * (wind_base[1] + jnp.sum(amplitude * jnp.sin(angle), axis=0))
    layers = thickness.shape[0]
    wave = (WAVE_LIMIT / layers) * jnp.sum(thickness, axis=0)
    depth_u = jnp.sum((thickness + east(thickness)) * 0.5, axis=0)
    depth_v = jnp.sum((thickness + north(thickness)) * 0.5, axis=0)
    surface, flow_u, flow_v = height, transport_u, transport_v
    thick, speed_u, speed_v = thickness, velocity_u, velocity_v
    for outer in range(STEPS):
        mean_u = jnp.zeros_like(surface)
        mean_v = jnp.zeros_like(surface)
        for inner in range(NSUB):
            surface = surface - (flow_u - west(flow_u) + flow_v - south(flow_v))
            flow_u = mask_u * (flow_u - wave * (east(surface) - surface) + stress_x)
            flow_v = mask_v * (flow_v - wave * (north(surface) - surface) + stress_y)
            mean_u = mean_u + flow_u
            mean_v = mean_v + flow_v
        mean_u = mean_u / NSUB
        mean_v = mean_v / NSUB
        thick_u = (thick + east(thick)) * 0.5
        thick_v = (thick + north(thick)) * 0.5
        flux_u = speed_u * thick_u
        flux_v = speed_v * thick_v
        pressure = jnp.cumsum(thick, axis=0)
        trial_u = speed_u - PRESS_COEF * (east(pressure) - pressure)
        trial_v = speed_v - PRESS_COEF * (north(pressure) - pressure)
        speed_u = mask_u * (trial_u + (mean_u - jnp.sum(thick_u * trial_u, axis=0)) / depth_u)
        speed_v = mask_v * (trial_v + (mean_v - jnp.sum(thick_v * trial_v, axis=0)) / depth_v)
        thick = thick - FLUX_STEP * (flux_u - west(flux_u) + flux_v - south(flux_v))
    return surface, flow_u, flow_v, thick, speed_u, speed_v
```

```python
import functools
import math

import jax
import jax.numpy as jnp
from jax import lax
from jax.experimental import pallas as pl
from jax.experimental.pallas import tpu as pltpu
from jax.sharding import PartitionSpec as P

NSUB = 6
STEPS = 2
MARGIN = NSUB
PAD = 8

WAVE_LIMIT = 0.225
STRESS_SCALE = 0.1
FLUX_STEP = 0.05
PRESS_COEF = 0.05
LANES = 128
VMEM_BYTES = 67043328
SPARE = 1 << 15
FIELDS = 8
SLOT = LANES // FIELDS
WEST = (NSUB - 1, NSUB, NSUB - 1, NSUB - 1, NSUB - 2, NSUB - 1, NSUB - 1, NSUB - 2)
EAST = (NSUB, NSUB, NSUB) + (NSUB - 1,) * 5
ORDER = (0, 1, 2, 3, 4, 6, 7, 5)
CUT = 32
PIECES = 2
MESH = pl.DeviceIdType.MESH


def roll(value, shift, axis):
    return pltpu.roll(value, shift % value.shape[axis], axis)


def iota(shape, axis):
    return lax.broadcasted_iota(jnp.int32, shape, axis)


def turns(seed, index, total):
    part = seed * index * (1.0 / total)
    angle = (2.0 * math.pi) * (part - jnp.floor(part))
    return jnp.cos(angle), jnp.sin(angle)


def tile_up(count):
    return -(-count // 8) * 8


def layer_trial(h_ref, u_ref, v_ref, o_h, o_u, o_v, sums, deep):
    layers, nx, ny = h_ref.shape
    at_east = iota((nx, ny), 0) == nx - 1
    at_north = iota((nx, ny), 1) == ny - 1
    zero = jnp.zeros((nx, ny), jnp.float32)
    press_u, press_v, sum_u, sum_v = zero, zero, zero, zero
    deep_u, deep_v = zero, zero
    for l in range(layers):
        h, u, v = h_ref[l], u_ref[l], v_ref[l]
        h_east, h_north = roll(h, -1, 0), roll(h, -1, 1)
        hu = (h + h_east) * 0.5
        hv = (h + h_north) * 0.5
        if deep:
            deep_u = deep_u + hu
            deep_v = deep_v + hv
        flux_u = jnp.where(at_east, 0.0, u * hu)
        flux_v = jnp.where(at_north, 0.0, v * hv)
        press_u = press_u + (h_east - h)
        press_v = press_v + (h_north - h)
        trial_u = u - PRESS_COEF * press_u
        trial_v = v - PRESS_COEF * press_v
        sum_u = sum_u + hu * trial_u
        sum_v = sum_v + hv * trial_v
        o_u[l] = trial_u
        o_v[l] = trial_v
        o_h[l] = h - FLUX_STEP * (flux_u - roll(flux_u, 1, 0) + flux_v - roll(flux_v, 1, 1))
    sums[0] = sum_u
    sums[1] = sum_v
    if deep:
        sums[2] = deep_u
        sums[3] = deep_v


def layer_edges(h_ref, v_ref, own_r, own_l, recv_w, recv_e, packs, o_h, o_u, o_v, sums, top, deep):
    layers, nx, ny = h_ref.shape
    up = own_l.shape[0]
    layer = iota((up, ny), 0)
    h_last, u_last, h_first = own_r[0:up], own_r[up:], own_l[...]
    h_e, h_w, u_w = recv_e[...], recv_w[0:up], recv_w[up:]
    hu = (h_last + h_e) * 0.5
    press = h_e - h_last
    step = 1
    while step < layers:
        press = press + jnp.where(layer >= step, roll(press, step, 0), 0.0)
        step *= 2
    trial = u_last - PRESS_COEF * press
    outflow = FLUX_STEP * (u_last * hu)
    inflow = FLUX_STEP * (u_w * ((h_w + h_first) * 0.5))
    whole = lambda a: jnp.sum(jnp.where(layer < layers, a, 0.0), axis=0, keepdims=True)
    sums[0, nx - 1 : nx, :] = whole(hu * trial)
    if deep:
        sums[2, nx - 1 : nx, :] = whole(hu)
    for l in range(layers):
        o_u[l, nx - 1 : nx, :] = trial[l : l + 1]
        o_h[l, nx - 1 : nx, :] = o_h[l, nx - 1 : nx, :] - outflow[l : l + 1]
        o_h[l, 0:1, :] = o_h[l, 0:1, :] + inflow[l : l + 1]

    lane = iota((nx, LANES), 1)
    last = ny - LANES
    at_end = lane == LANES - 1
    at_start = jnp.logical_and(top, lane == 0)
    side = packs[0]
    cap = jnp.where(top, packs[1], side)
    press, total, deep_v = 0.0, 0.0, 0.0
    for l in range(layers):
        h, v = h_ref[l, :, last:ny], v_ref[l, :, last:ny]
        h_north = roll(cap, LANES - 1 - l, 1)
        hv = (h + h_north) * 0.5
        press = press + (h_north - h)
        trial = v - PRESS_COEF * press
        total = total + hv * trial
        deep_v = deep_v + hv
        o_v[l, :, last:ny] = jnp.where(at_end, trial, o_v[l, :, last:ny])
        o_h[l, :, last:ny] = o_h[l, :, last:ny] - jnp.where(at_end, FLUX_STEP * (v * hv), 0.0)
        h_south, v_south = roll(side, -l, 1), roll(side, -(layers + l), 1)
        inflow = FLUX_STEP * (v_south * ((h_south + h_ref[l, :, 0:LANES]) * 0.5))
        o_h[l, :, 0:LANES] = o_h[l, :, 0:LANES] + jnp.where(at_start, inflow, 0.0)
    sums[1, :, last:ny] = jnp.where(at_end, total, sums[1, :, last:ny])
    if deep:
        sums[3, :, last:ny] = jnp.where(at_end, deep_v, sums[3, :, last:ny])


def layer_close(o_u, o_v, sums, mean, masks, depth, deep):
    if deep:
        depth[0] = 1.0 / sums[2]
        depth[1] = 1.0 / sums[3]
    for k, out in enumerate((o_u, o_v)):
        fix = (mean[k] * (1.0 / NSUB) - sums[k]) * depth[k]
        mask = masks[k]
        for l in range(out.shape[0]):
            out[l] = mask * (out[l] + fix)


def last_kernel(flat, n_h, n_u, n_v, o_eta, o_bu, o_bv, o_h, o_u, o_v, sems):
    layers = n_h.shape[0]
    moves = [(flat.at[k], o) for k, o in enumerate((o_eta, o_bu, o_bv))]
    cut = layers // PIECES
    for n, o in ((n_h, o_h), (n_u, o_u), (n_v, o_v)):
        for p in range(PIECES):
            part = slice(p * cut, layers if p == PIECES - 1 else (p + 1) * cut)
            moves.append((n.at[part], o.at[part]))
    copies = [pltpu.make_async_copy(src, dst, sems.at[k]) for k, (src, dst) in enumerate(moves)]
    for copy in copies:
        copy.start()
    for copy in copies:
        copy.wait()


def kernel(
    zonal_devices,
    merid_devices,
    height_any,
    trans_u_any,
    trans_v_any,
    thick_any,
    vel_u_any,
    vel_v_any,
    faces_any,
    seeds_any,
    scale_any,
    base_any,
    flat,
    o_h,
    o_u,
    o_v,
    thick,
    vel_u,
    vel_v,
    faces,
    seeds,
    scale,
    mid_h,
    mid_u,
    mid_v,
    mean,
    sums,
    depth,
    X,
    G,
    D,
    F,
    wind_own,
    wind_far,
    west_send,
    west_recv,
    east_send,
    east_recv,
    pack_send,
    inner_recv,
    fold_recv,
    lay_send_r,
    lay_send_l,
    lay_recv_w,
    lay_recv_e,
    lay_pack_send,
    lay_pack_recv,
    load_sem,
    send_sem,
    recv_sem,
    lay_send_sem,
    lay_recv_sem,
    late_sem,
):
    layers, nx, ny = thick.shape
    Z = zonal_devices
    total_x, total_y = nx * Z, ny * merid_devices
    z = lax.axis_index("zonal")
    m = lax.axis_index("merid")
    other = 1 - m
    bottom = m == 0
    top = m == merid_devices - 1
    right, left = lax.rem(z + 1, Z), lax.rem(z + Z - 1, Z)
    mirror = Z - 1 - z
    mirror_e, mirror_w = lax.rem(mirror + 1, Z), lax.rem(mirror + Z - 1, Z)
    rows = nx + 2 * PAD
    width = ny + LANES
    last = ny - LANES
    own = slice(PAD, PAD + nx)
    lane = iota((nx, LANES), 1)

    barrier = pltpu.get_barrier_semaphore()
    first_z, last_z = z == 0, z == Z - 1
    mirrors = (mirror_w, mirror, mirror_e)

    def greet(sem, zz, mm):
        pl.semaphore_signal(sem, inc=1, device_id={"zonal": zz, "merid": mm}, device_id_type=MESH)

    greet(barrier, z, other)
    for mm in (m, other):
        greet(barrier, left, mm)

        @pl.when(jnp.logical_not(last_z))
        def _():
            greet(barrier, right, mm)

    for zz in mirrors:

        @pl.when(jnp.logical_and(top, zz > z))
        def _():
            greet(barrier, zz, m)

    moves = (
        (faces_any, faces),
        (height_any, X.at[0, own, 0:ny]),
        (trans_u_any, X.at[1, own, 0:ny]),
        (trans_v_any, X.at[2, own, 0:ny]),
        (base_any, X.at[6:8, own, 0:ny]),
        (thick_any, thick),
        (vel_u_any, vel_u),
        (vel_v_any, vel_v),
        (seeds_any, seeds),
        (scale_any, scale),
    )
    loads = [pltpu.make_async_copy(src, dst, load_sem.at[k]) for k, (src, dst) in enumerate(moves)]
    for load in loads:
        load.start()

    near = 3 + jnp.where(first_z, 0, 2)
    lower = sum((zz < z).astype(jnp.int32) for zz in mirrors)
    upper = sum((zz > z).astype(jnp.int32) for zz in mirrors)
    pl.semaphore_wait(barrier, near + jnp.where(top, lower, 0))

    @pl.when(last_z)
    def _():
        for mm in (m, other):
            greet(late_sem.at[0], right, mm)

    for zz in mirrors:

        @pl.when(jnp.logical_and(top, zz < z))
        def _():
            greet(late_sem.at[1], zz, m)

    loads[0].wait()
    X[3, own, 0:ny] = faces[0].astype(jnp.float32)
    X[4, own, 0:ny] = faces[1].astype(jnp.float32)
    for load in loads[1:5]:
        load.wait()

    def pack_rows(step, start, stop):
        west = sum(WEST[f] for f in ORDER[:start])
        east = sum(EAST[f] for f in ORDER[:start])
        for f in ORDER[start:stop]:
            west_send[step, west : west + WEST[f], :] = X[f, PAD + nx - WEST[f] : PAD + nx, 0:ny]
            east_send[step, east : east + EAST[f], :] = X[f, PAD : PAD + EAST[f], 0:ny]
            west += WEST[f]
            east += EAST[f]

    def pack_edges(step, fields):
        inner = jnp.zeros((nx, LANES), jnp.float32)
        crest = jnp.zeros((nx, LANES), jnp.float32)
        for f in range(fields):
            here = jnp.logical_and(lane >= f * SLOT, lane < (f + 1) * SLOT)
            high = roll(X[f, own, last:ny], SLOT * (f + 1), 1)
            low = roll(X[f, own, 0:LANES], SLOT * f, 1)
            crest = jnp.where(here, high, crest)
            inner = jnp.where(here, jnp.where(bottom, high, low), inner)
        pack_send[step, 0] = inner
        pack_send[step, 2] = crest
        for r in range(nx):
            pack_send[step, 1, r : r + 1, :] = pack_send[step, 2, nx - 1 - r : nx - r, :]

    def send_tile(step, fields):
        def send(src, dst, k, zz, mm):
            return pltpu.make_async_remote_copy(
                src_ref=src,
                dst_ref=dst,
                send_sem=send_sem.at[step, k],
                recv_sem=recv_sem.at[step, k],
                device_id={"zonal": zz, "merid": mm},
                device_id_type=MESH,
            )

        def rows_of(src, dst, k, zz, count):
            cuts = [0, CUT, count] if count > CUT else [0, count]
            parts = [slice(low, high) for low, high in zip(cuts[:-1], cuts[1:])]
            return [send(src.at[step, p], dst.at[step, p], k + 2 * n, zz, m) for n, p in enumerate(parts)]

        tail, whole, start = slice(nx - PAD, nx), slice(0, nx), slice(0, PAD)
        places = (slice(0, PAD), own, slice(PAD + nx, rows))
        inner = lambda s, part: (pack_send.at[step, 0, part], inner_recv.at[step, places[s]])
        west = rows_of(west_send, west_recv, 0, right, tile_up(sum(WEST[:fields])))
        east = rows_of(east_send, east_recv, 1, left, tile_up(sum(EAST[:fields])))
        west.append(send(*inner(0, tail), 6, right, other))
        east.append(send(*inner(2, start), 4, left, other))
        across = send(*inner(1, whole), 5, z, other)
        folds = []
        for s, part, zz in ((2, start, mirror_w), (1, whole, mirror), (0, tail, mirror_e)):
            src, dst = pack_send.at[step, 1, part], fold_recv.at[step, places[s]]
            near = pltpu.make_async_copy(src, dst, recv_sem.at[step, 7 + s])
            folds.append((send(src, dst, 7 + s, zz, m), near, zz))
        return west, east, across, folds

    even = lax.rem(z, 2) == 0

    def start_all(copies):
        for copy in copies:
            copy.start()

    far_west, far_east = jnp.logical_not(even), jnp.logical_and(even, jnp.logical_not(first_z))

    def each(west_when, east_when, act, tile):
        pl.when(west_when)(lambda: act(tile[0]))
        pl.when(east_when)(lambda: act(tile[1]))

    def start_folds(folds, chosen):
        for far_copy, _, zz in folds:
            pl.when(jnp.logical_and(top, chosen(zz)))(far_copy.start)

    def take_tile(step, fields, west_copies, east_copies, across, folds):
        for copy in west_copies + east_copies + [across]:
            copy.wait()
        for far_copy, near_copy, zz in folds:

            @pl.when(jnp.logical_and(top, zz != z))
            def _():
                far_copy.wait()

            @pl.when(jnp.logical_and(top, zz == z))
            def _():
                near_copy.wait()

        west = east = 0
        for f in ORDER[:fields]:
            X[f, PAD - WEST[f] : PAD, 0:ny] = west_recv[step, west : west + WEST[f], :]
            X[f, PAD + nx : PAD + nx + EAST[f], 0:ny] = east_recv[step, east : east + EAST[f], :]
            west += WEST[f]
            east += EAST[f]
        for f in range(fields):
            got = inner_recv[step]
            X[f, :, ny:width] = jnp.where(
                top, roll(got, LANES - SLOT * (f + 1), 1), roll(got, LANES - SLOT * f, 1)
            )
            G[f] = roll(fold_recv[step], LANES - SLOT * (f + 1), 1)

    pack_rows(0, 0, FIELDS - 1)
    tile = send_tile(0, FIELDS)
    lead = (jnp.logical_or(far_west, first_z), far_east)
    each(*lead, lambda c: c[0].start(), tile)
    loads[5].wait()
    total = thick[0]
    for l in range(1, layers):
        total = total + thick[l]
    X[5, own, 0:ny] = (WAVE_LIMIT / layers) * total
    pack_rows(0, FIELDS - 1, FIELDS)
    pack_edges(0, FIELDS)
    each(*lead, lambda c: start_all(c[1:]), tile)
    each(far_east, far_west, start_all, tile)
    tile[2].start()
    start_folds(tile[3], lambda zz: zz < z)
    for _, near_copy, zz in tile[3]:
        pl.when(jnp.logical_and(top, zz == z))(near_copy.start)

    def lay_copies(step):
        def one(src, dst, k, zz, mm):
            return pltpu.make_async_remote_copy(
                src_ref=src,
                dst_ref=dst,
                send_sem=lay_send_sem.at[step, k],
                recv_sem=lay_recv_sem.at[step, k],
                device_id={"zonal": zz, "merid": mm},
                device_id_type=MESH,
            )

        return [
            one(lay_send_r.at[step], lay_recv_w.at[step], 0, right, m),
            one(lay_send_l.at[step], lay_recv_e.at[step], 1, left, m),
            one(lay_pack_send.at[step, 0], lay_pack_recv.at[step, 0], 2, z, other),
            one(lay_pack_send.at[step, 1], lay_pack_recv.at[step, 1], 3, mirror, m),
        ]

    above = lay_send_r.shape[1] // 2

    def send_layers(step, h_ref, u_ref, v_ref):
        edge = jnp.zeros((nx, LANES), jnp.float32)
        brim = jnp.zeros((nx, LANES), jnp.float32)
        for l in range(layers):
            lay_send_r[step, l : l + 1, :] = h_ref[l, nx - 1 : nx, :]
            lay_send_r[step, above + l : above + l + 1, :] = u_ref[l, nx - 1 : nx, :]
            lay_send_l[step, l : l + 1, :] = h_ref[l, 0:1, :]
            high = roll(h_ref[l, :, last:ny], l + 1, 1)
            low = roll(h_ref[l, :, 0:LANES], l, 1)
            high_v = roll(v_ref[l, :, last:ny], layers + l + 1, 1)
            edge = jnp.where(lane == l, jnp.where(bottom, high, low), edge)
            edge = jnp.where(lane == layers + l, high_v, edge)
            brim = jnp.where(lane == l, high, brim)
        lay_pack_send[step, 0] = edge
        lay_pack_send[step, 2] = brim
        for r in range(nx):
            lay_pack_send[step, 1, r : r + 1, :] = lay_pack_send[step, 2, nx - 1 - r : nx - r, :]
        return lay_copies(step)

    def start_layers(out, first):
        out[2].start()
        late_left, late_fold = (first_z, mirror > z) if first else (False, False)
        pl.when(jnp.logical_and(top, jnp.logical_not(late_fold)))(out[3].start)
        pl.when(far_west)(lambda: start_all(out[:2]))
        pl.when(jnp.logical_and(even, jnp.logical_not(late_left)))(lambda: start_all(out[1::-1]))
        if first:
            pl.when(first_z)(out[0].start)

    def wait_layers(out):
        for copy in out[:3]:
            copy.wait()

        @pl.when(top)
        def _():
            out[3].wait()

    for load in loads[6:]:
        load.wait()
    out = send_layers(0, thick, vel_u, vel_v)

    start_layers(out, True)
    first = (z * nx - PAD).astype(jnp.float32)
    col = first + iota((rows, 1), 0).astype(jnp.float32) + float(total_x)
    far_col = float(2 * total_x - 1) - (first + iota((rows, 1), 0).astype(jnp.float32))
    spot = iota((1, width), 1)
    row = spot + m * ny
    row = jnp.where(jnp.logical_and(top, spot >= ny), row - width, row).astype(jnp.float32)
    far_row = (iota((1, LANES), 1) + (total_y - LANES)).astype(jnp.float32)
    px = jnp.zeros((rows, width), jnp.float32)
    py = jnp.zeros((rows, width), jnp.float32)
    fx = jnp.zeros((rows, LANES), jnp.float32)
    fy = jnp.zeros((rows, LANES), jnp.float32)
    for k in range(seeds.shape[1]):
        seed_x = seeds[0, k].astype(jnp.float32)
        seed_y = seeds[1, k].astype(jnp.float32)
        ca, sa = turns(seed_x, col, total_x)
        cf, sf = turns(seed_x, far_col, total_x)
        cb, sb = turns(seed_y, row, total_y)
        cg, sg = turns(seed_y, far_row, total_y)
        amp = scale[k]
        ca, sa, cf, sf = amp * ca, amp * sa, amp * cf, amp * sf
        px = px + (ca * cb - sa * sb)
        py = py + (sa * cb + ca * sb)
        fx = fx + (cf * cg - sf * sg)
        fy = fy + (sf * cg + cf * sg)
    wind_own[0] = px
    wind_own[1] = py
    wind_far[0] = fx
    wind_far[1] = fy

    layer_trial(thick, vel_u, vel_v, mid_h, mid_u, mid_v, sums, True)

    @pl.when(first_z)
    def _():
        pl.semaphore_wait(late_sem.at[0], 2)
        start_all(tile[1])


    @pl.when(jnp.logical_and(top, upper > 0))
    def _():
        pl.semaphore_wait(late_sem.at[1], upper)

    start_folds(tile[3], lambda zz: zz > z)
    pl.when(first_z)(out[1].start)
    pl.when(jnp.logical_and(top, mirror > z))(out[3].start)

    take_tile(0, FIELDS, *tile)
    for k in range(2):
        X[6 + k] = STRESS_SCALE * (X[6 + k] + wind_own[k])
        G[6 + k] = STRESS_SCALE * (G[6 + k] + wind_far[k])

    lanes = iota((rows, width), 1)
    wall = jnp.logical_and(bottom, lanes == 0)
    crown = jnp.logical_and(top, lanes == ny - 1)
    far_top = iota((rows, LANES), 1) == LANES - 1

    def close_step(step, h_ref, v_ref, n_h, n_u, n_v):
        layer_edges(
            h_ref, v_ref, lay_send_r.at[step], lay_send_l.at[step], lay_recv_w.at[step], lay_recv_e.at[step],
            lay_pack_recv.at[step], n_h, n_u, n_v, sums, top, step == 0,
        )
        layer_close(n_u, n_v, sums, mean, masks, depth, step == 0)

    def substep(carry):
        eta, bu, bv, south_v, g_eta, g_bu, g_bv, g_south_v = carry
        eta = eta - (bu - roll(bu, 1, 0) + bv - south_v)
        g_eta = g_eta - (g_bu - roll(g_bu, -1, 0) + g_bv - g_south_v)
        north, south = roll(eta, -1, 1), roll(eta, 1, 1)
        north = jnp.where(crown, g_eta[:, LANES - 1 :], north)
        g_north = jnp.where(far_top, eta[:, ny - 1 : ny], roll(g_eta, -1, 1))
        g_south = roll(g_eta, 1, 1)
        bu = X[3] * (bu - X[5] * (roll(eta, -1, 0) - eta) + X[6])
        bv = X[4] * (bv - X[5] * (north - eta) + X[7])
        south_v = jnp.where(wall, 0.0, D[0] * (south_v - D[1] * (eta - south) + D[2]))
        g_bu = G[3] * (g_bu - G[5] * (roll(g_eta, 1, 0) - g_eta) + G[6])
        g_bv = G[4] * (g_bv - G[5] * (g_north - g_eta) + G[7])
        g_south_v = F[0] * (g_south_v - F[1] * (g_eta - g_south) + F[2])
        mean[0] = mean[0] + bu[own, 0:ny]
        mean[1] = mean[1] + bv[own, 0:ny]
        return eta, bu, bv, south_v, g_eta, g_bu, g_bv, g_south_v

    def substeps():
        mean[...] = jnp.zeros((2, nx, ny), jnp.float32)
        bv, g_bv = X[2], G[2]
        carry = X[0], X[1], bv, jnp.where(wall, 0.0, roll(bv, 1, 1)), G[0], G[1], g_bv, roll(g_bv, 1, 1)
        for _ in range(NSUB):
            carry = substep(carry)
        for k in range(3):
            X[k] = carry[k]
            G[k] = carry[4 + k]

    for k, f in enumerate((4, 5, 7)):
        D[k] = roll(X[f], 1, 1)
        F[k] = roll(G[f], 1, 1)
    masks = X[3, own, 0:ny], X[4, own, 0:ny]
    h_ref, u_ref, v_ref = thick, vel_u, vel_v
    n_h, n_u, n_v = mid_h, mid_u, mid_v
    for step in range(STEPS - 1):
        substeps()
        pack_rows(step + 1, 0, 3)
        tile = send_tile(step + 1, 3)
        lead = (far_west, even)
        each(*lead, lambda c: start_all(c[:-1]), tile)
        pack_edges(step + 1, 3)
        each(*lead, lambda c: c[-1].start(), tile)
        tile[2].start()
        start_folds(tile[3], lambda zz: zz != z)
        for _, near_copy, zz in tile[3]:
            pl.when(jnp.logical_and(top, zz == z))(near_copy.start)
        each(even, far_west, start_all, tile)
        wait_layers(out)
        close_step(step, h_ref, v_ref, n_h, n_u, n_v)
        h_ref, u_ref, v_ref = n_h, n_u, n_v
        n_h, n_u, n_v = o_h, o_u, o_v
        out = send_layers(step + 1, h_ref, u_ref, v_ref)
        start_layers(out, False)
        layer_trial(h_ref, u_ref, v_ref, n_h, n_u, n_v, sums, False)
        take_tile(step + 1, 3, *tile)
    substeps()
    for f in range(3):
        flat[f] = X[f, own, 0:ny]
    wait_layers(out)
    close_step(STEPS - 1, h_ref, v_ref, n_h, n_u, n_v)


def body(zonal_devices, merid_devices, *args):
    thickness = args[3]
    layers, nx, ny = thickness.shape
    up = tile_up(layers)
    f32 = jnp.float32
    vmem = pl.BlockSpec(memory_space=pltpu.VMEM)
    far = pl.BlockSpec(memory_space=pltpu.HBM)
    hbm = pl.BlockSpec(memory_space=pl.ANY)
    rows = nx + 2 * PAD
    west, east = tile_up(sum(WEST)), tile_up(sum(EAST))
    plane = jax.ShapeDtypeStruct((nx, ny), f32)
    solid = jax.ShapeDtypeStruct((layers, nx, ny), f32)
    kept = [(3, nx, ny), (layers, nx, ny), (layers, nx, ny), (layers, nx, ny)]
    room = sum(math.prod(shape) for shape in kept)
    args = list(args)
    args[7] = args[7].T
    between = pl.pallas_call(
        functools.partial(kernel, zonal_devices, merid_devices),
        out_shape=[pltpu.VMEM(shape, f32) for shape in kept],
        in_specs=[far] * 10,
        out_specs=[vmem] * len(kept),
        scratch_shapes=[
            pltpu.VMEM((layers, nx, ny), f32),
            pltpu.VMEM((layers, nx, ny), f32),
            pltpu.VMEM((layers, nx, ny), f32),
            pltpu.VMEM((2, nx, ny), jnp.int32),
            pltpu.SMEM(args[7].shape, jnp.int32),
            pltpu.SMEM(args[8].shape, f32),
            pltpu.VMEM((layers, nx, ny), f32),
            pltpu.VMEM((layers, nx, ny), f32),
            pltpu.VMEM((layers, nx, ny), f32),
            pltpu.VMEM((2, nx, ny), f32),
            pltpu.VMEM((4, nx, ny), f32),
            pltpu.VMEM((2, nx, ny), f32),
            pltpu.VMEM((FIELDS, rows, ny + LANES), f32),
            pltpu.VMEM((FIELDS, rows, LANES), f32),
            pltpu.VMEM((3, rows, ny + LANES), f32),
            pltpu.VMEM((3, rows, LANES), f32),
            pltpu.VMEM((2, rows, ny + LANES), f32),
            pltpu.VMEM((2, rows, LANES), f32),
            pltpu.VMEM((STEPS, west, ny), f32),
            pltpu.VMEM((STEPS, west, ny), f32),
            pltpu.VMEM((STEPS, east, ny), f32),
            pltpu.VMEM((STEPS, east, ny), f32),
            pltpu.VMEM((STEPS, 3, nx, LANES), f32),
            pltpu.VMEM((STEPS, rows, LANES), f32),
            pltpu.VMEM((STEPS, rows, LANES), f32),
            pltpu.VMEM((STEPS, 2 * up, ny), f32),
            pltpu.VMEM((STEPS, up, ny), f32),
            pltpu.VMEM((STEPS, 2 * up, ny), f32),
            pltpu.VMEM((STEPS, up, ny), f32),
            pltpu.VMEM((STEPS, 3, nx, LANES), f32),
            pltpu.VMEM((STEPS, 2, nx, LANES), f32),
            pltpu.SemaphoreType.DMA((10,)),
            pltpu.SemaphoreType.DMA((STEPS, 10)),
            pltpu.SemaphoreType.DMA((STEPS, 10)),
            pltpu.SemaphoreType.DMA((STEPS, 4)),
            pltpu.SemaphoreType.DMA((STEPS, 4)),
            pltpu.SemaphoreType.REGULAR((2,)),
        ],
        compiler_params=pltpu.CompilerParams(
            collective_id=0, has_side_effects=True, vmem_limit_bytes=VMEM_BYTES - 4 * room - SPARE
        ),
        name="ocean",
    )(*args)
    return pl.pallas_call(
        last_kernel,
        out_shape=(plane, plane, plane, solid, solid, solid),
        in_specs=[vmem] * len(kept),
        out_specs=[hbm] * 6,
        scratch_shapes=[pltpu.SemaphoreType.DMA((3 + 3 * PIECES,))],
        compiler_params=pltpu.CompilerParams(vmem_limit_bytes=24 * 1024 * 1024),
        name="last",
    )(*between)


def solution(mesh):
    field = P(("members", "zonal"), "merid")
    solid = P(None, ("members", "zonal"), "merid")
    fixed = P(None, "zonal", "merid")
    return jax.shard_map(
        functools.partial(body, mesh.shape["zonal"], mesh.shape["merid"]),
        mesh=mesh,
        in_specs=(
            field, field, field, solid, solid, solid, fixed, P("members", None), P("members"), fixed,
        ),
        out_specs=(field, field, field, solid, solid, solid),
        check_vma=False,
    )
```

```python
import functools
import math

import jax
import jax.numpy as jnp
from jax import lax
from jax.experimental import pallas as pl
from jax.experimental.pallas import tpu as pltpu
from jax.sharding import PartitionSpec as P

NSUB = 6
STEPS = 2
MARGIN = NSUB
PAD = 8

WAVE_LIMIT = 0.225
STRESS_SCALE = 0.1
FLUX_STEP = 0.05
PRESS_COEF = 0.05
LANES = 128
VMEM_BYTES = 67043328
SPARE = 1 << 15
FIELDS = 8
SLOT = LANES // FIELDS
WEST = (NSUB - 1, NSUB, NSUB - 1, NSUB - 1, NSUB - 2, NSUB - 1, NSUB - 1, NSUB - 2)
EAST = (NSUB, NSUB, NSUB) + (NSUB - 1,) * 5
ORDER = (0, 1, 2, 3, 4, 6, 7, 5)
CUT = 32
MESH = pl.DeviceIdType.MESH


def roll(value, shift, axis):
    return pltpu.roll(value, shift % value.shape[axis], axis)


def iota(shape, axis):
    return lax.broadcasted_iota(jnp.int32, shape, axis)


def turns(seed, index, total):
    part = seed * index * (1.0 / total)
    angle = (2.0 * math.pi) * (part - jnp.floor(part))
    return jnp.cos(angle), jnp.sin(angle)


def lines(ref):
    return math.prod(ref.shape) // LANES


def drain(ref, sem):
    pltpu.make_async_copy(ref, ref, sem).wait()


def tile_up(count):
    return -(-count // 8) * 8


def layer_trial(h_ref, u_ref, v_ref, o_h, o_u, o_v, sums, deep):
    layers, nx, ny = h_ref.shape
    at_east = iota((nx, ny), 0) == nx - 1
    at_north = iota((nx, ny), 1) == ny - 1
    zero = jnp.zeros((nx, ny), jnp.float32)
    press_u, press_v, sum_u, sum_v = zero, zero, zero, zero
    deep_u, deep_v = zero, zero
    for l in range(layers):
        h, u, v = h_ref[l], u_ref[l], v_ref[l]
        h_east, h_north = roll(h, -1, 0), roll(h, -1, 1)
        hu = (h + h_east) * 0.5
        hv = (h + h_north) * 0.5
        if deep:
            deep_u = deep_u + hu
            deep_v = deep_v + hv
        flux_u = jnp.where(at_east, 0.0, u * hu)
        flux_v = jnp.where(at_north, 0.0, v * hv)
        press_u = press_u + (h_east - h)
        press_v = press_v + (h_north - h)
        trial_u = u - PRESS_COEF * press_u
        trial_v = v - PRESS_COEF * press_v
        sum_u = sum_u + hu * trial_u
        sum_v = sum_v + hv * trial_v
        o_u[l] = trial_u
        o_v[l] = trial_v
        o_h[l] = h - FLUX_STEP * (flux_u - roll(flux_u, 1, 0) + flux_v - roll(flux_v, 1, 1))
    sums[0] = sum_u
    sums[1] = sum_v
    if deep:
        sums[2] = deep_u
        sums[3] = deep_v


def layer_edges(h_ref, v_ref, own_r, own_l, recv_w, recv_e, packs, o_h, o_u, o_v, sums, top, deep):
    layers, nx, ny = h_ref.shape
    up = own_l.shape[0]
    layer = iota((up, ny), 0)
    h_last, u_last, h_first = own_r[0:up], own_r[up:], own_l[...]
    h_e, h_w, u_w = recv_e[...], recv_w[0:up], recv_w[up:]
    hu = (h_last + h_e) * 0.5
    press = h_e - h_last
    step = 1
    while step < layers:
        press = press + jnp.where(layer >= step, roll(press, step, 0), 0.0)
        step *= 2
    trial = u_last - PRESS_COEF * press
    outflow = FLUX_STEP * (u_last * hu)
    inflow = FLUX_STEP * (u_w * ((h_w + h_first) * 0.5))
    whole = lambda a: jnp.sum(jnp.where(layer < layers, a, 0.0), axis=0, keepdims=True)
    sums[0, nx - 1 : nx, :] = whole(hu * trial)
    if deep:
        sums[2, nx - 1 : nx, :] = whole(hu)
    for l in range(layers):
        o_u[l, nx - 1 : nx, :] = trial[l : l + 1]
        o_h[l, nx - 1 : nx, :] = o_h[l, nx - 1 : nx, :] - outflow[l : l + 1]
        o_h[l, 0:1, :] = o_h[l, 0:1, :] + inflow[l : l + 1]

    lane = iota((nx, LANES), 1)
    last = ny - LANES
    at_end = lane == LANES - 1
    at_start = jnp.logical_and(top, lane == 0)
    side = packs[0]
    cap = jnp.where(top, packs[1], side)
    press, total, deep_v = 0.0, 0.0, 0.0
    for l in range(layers):
        h, v = h_ref[l, :, last:ny], v_ref[l, :, last:ny]
        h_north = roll(cap, LANES - 1 - l, 1)
        hv = (h + h_north) * 0.5
        press = press + (h_north - h)
        trial = v - PRESS_COEF * press
        total = total + hv * trial
        deep_v = deep_v + hv
        o_v[l, :, last:ny] = jnp.where(at_end, trial, o_v[l, :, last:ny])
        o_h[l, :, last:ny] = o_h[l, :, last:ny] - jnp.where(at_end, FLUX_STEP * (v * hv), 0.0)
        h_south, v_south = roll(side, -l, 1), roll(side, -(layers + l), 1)
        inflow = FLUX_STEP * (v_south * ((h_south + h_ref[l, :, 0:LANES]) * 0.5))
        o_h[l, :, 0:LANES] = o_h[l, :, 0:LANES] + jnp.where(at_start, inflow, 0.0)
    sums[1, :, last:ny] = jnp.where(at_end, total, sums[1, :, last:ny])
    if deep:
        sums[3, :, last:ny] = jnp.where(at_end, deep_v, sums[3, :, last:ny])


def layer_close(o_u, o_v, sums, mean, masks, depth, deep):
    if deep:
        depth[0] = 1.0 / sums[2]
        depth[1] = 1.0 / sums[3]
    for k, out in enumerate((o_u, o_v)):
        fix = (mean[k] * (1.0 / NSUB) - sums[k]) * depth[k]
        mask = masks[k]
        for l in range(out.shape[0]):
            out[l] = mask * (out[l] + fix)


def last_kernel(flat, n_h, n_u, n_v, o_eta, o_bu, o_bv, o_h, o_u, o_v, sems):
    moves = [(flat.at[k], o, 0) for k, o in enumerate((o_eta, o_bu, o_bv))]
    moves += [(n_h, o_h, 1), (n_u, o_u, 2), (n_v, o_v, 3)]
    copies = [pltpu.make_async_copy(src, dst, sems.at[k]) for src, dst, k in moves]
    for copy in copies:
        copy.start()
    drain(flat, sems.at[0])
    for copy in copies[3:]:
        copy.wait()


def kernel(
    zonal_devices,
    merid_devices,
    height_any,
    trans_u_any,
    trans_v_any,
    thick_any,
    vel_u_any,
    vel_v_any,
    faces_any,
    seeds_any,
    scale_any,
    base_any,
    flat,
    o_h,
    o_u,
    o_v,
    thick,
    vel,
    faces,
    seeds,
    scale,
    mid_h,
    mid_u,
    mid_v,
    mean,
    sums,
    depth,
    X,
    G,
    D,
    F,
    wind_own,
    wind_far,
    west_send,
    west_recv,
    east_send,
    east_recv,
    pack_send,
    inner_recv,
    fold_recv,
    lay_send_r,
    lay_send_l,
    lay_recv_w,
    lay_recv_e,
    lay_pack_send,
    lay_pack_recv,
    blank,
    load_sem,
    send_sem,
    recv_sem,
    lay_recv_sem,
    late_sem,
):
    layers, nx, ny = thick.shape
    Z = zonal_devices
    total_x, total_y = nx * Z, ny * merid_devices
    z = lax.axis_index("zonal")
    m = lax.axis_index("merid")
    other = 1 - m
    bottom = m == 0
    top = m == merid_devices - 1
    right, left = lax.rem(z + 1, Z), lax.rem(z + Z - 1, Z)
    mirror = Z - 1 - z
    mirror_e, mirror_w = lax.rem(mirror + 1, Z), lax.rem(mirror + Z - 1, Z)
    rows = nx + 2 * PAD
    width = ny + LANES
    last = ny - LANES
    own = slice(PAD, PAD + nx)
    lane = iota((nx, LANES), 1)

    barrier = pltpu.get_barrier_semaphore()
    first_z, last_z = z == 0, z == Z - 1
    mirrors = (mirror_w, mirror, mirror_e)

    def greet(sem, zz, mm):
        pl.semaphore_signal(sem, inc=1, device_id={"zonal": zz, "merid": mm}, device_id_type=MESH)

    greet(barrier, z, other)
    for mm in (m, other):
        greet(barrier, left, mm)

        @pl.when(jnp.logical_not(last_z))
        def _():
            greet(barrier, right, mm)

    for zz in mirrors:

        @pl.when(jnp.logical_and(top, zz > z))
        def _():
            greet(barrier, zz, m)

    moves = (
        (faces_any, faces),
        (height_any, X.at[0, own, 0:ny]),
        (trans_u_any, X.at[1, own, 0:ny]),
        (trans_v_any, X.at[2, own, 0:ny]),
        (base_any, X.at[6:8, own, 0:ny]),
        (thick_any, thick),
        (vel_u_any, vel.at[0]),
        (vel_v_any, vel.at[1]),
        (seeds_any, seeds),
        (scale_any, scale),
    )
    group = (0, 0, 0, 0, 0, 1, 2, 2, 3, 4)
    vel_u, vel_v = vel.at[0], vel.at[1]
    loads = [pltpu.make_async_copy(src, dst, load_sem.at[k]) for k, (src, dst) in zip(group, moves)]
    for load in loads:
        load.start()

    near = 3 + jnp.where(first_z, 0, 2)
    lower = sum((zz < z).astype(jnp.int32) for zz in mirrors)
    upper = sum((zz > z).astype(jnp.int32) for zz in mirrors)
    pl.semaphore_wait(barrier, near + jnp.where(top, lower, 0))

    @pl.when(last_z)
    def _():
        for mm in (m, other):
            greet(late_sem.at[0], right, mm)

    for zz in mirrors:

        @pl.when(jnp.logical_and(top, zz < z))
        def _():
            greet(late_sem.at[1], zz, m)

    drain(blank.at[0 : sum(lines(dst) for _, dst in moves[:5])], load_sem.at[0])
    X[3, own, 0:ny] = faces[0].astype(jnp.float32)
    X[4, own, 0:ny] = faces[1].astype(jnp.float32)

    def pack_rows(step, start, stop):
        west = sum(WEST[f] for f in ORDER[:start])
        east = sum(EAST[f] for f in ORDER[:start])
        for f in ORDER[start:stop]:
            west_send[step, west : west + WEST[f], :] = X[f, PAD + nx - WEST[f] : PAD + nx, 0:ny]
            east_send[step, east : east + EAST[f], :] = X[f, PAD : PAD + EAST[f], 0:ny]
            west += WEST[f]
            east += EAST[f]

    def pack_edges(step, fields, between=lambda: None):
        inner = jnp.zeros((nx, LANES), jnp.float32)
        crest = jnp.zeros((nx, LANES), jnp.float32)
        for f in range(fields):
            here = jnp.logical_and(lane >= f * SLOT, lane < (f + 1) * SLOT)
            high = roll(X[f, own, last:ny], SLOT * (f + 1), 1)
            low = roll(X[f, own, 0:LANES], SLOT * f, 1)
            crest = jnp.where(here, high, crest)
            inner = jnp.where(here, jnp.where(bottom, high, low), inner)
        pack_send[step, 0] = inner
        between()
        pack_send[step, 2] = crest
        for r in range(nx):
            pack_send[step, 1, r : r + 1, :] = pack_send[step, 2, nx - 1 - r : nx - r, :]

    leaving = {}

    def send_tile(step, fields):
        def send(src, dst, k, zz, mm):
            leaving[k] = leaving.get(k, 0) + lines(src)
            return pltpu.make_async_remote_copy(
                src_ref=src,
                dst_ref=dst,
                send_sem=send_sem.at[k],
                recv_sem=recv_sem.at[step],
                device_id={"zonal": zz, "merid": mm},
                device_id_type=MESH,
            )

        def rows_of(src, dst, k, zz, count):
            cuts = [0, CUT, count] if count > CUT else [0, count]
            parts = [slice(low, high) for low, high in zip(cuts[:-1], cuts[1:])]
            return [send(src.at[step, p], dst.at[step, p], 0 if n else k, zz, m) for n, p in enumerate(parts)]

        tail, whole, start = slice(nx - PAD, nx), slice(0, nx), slice(0, PAD)
        places = (slice(0, PAD), own, slice(PAD + nx, rows))
        inner = lambda s, part: (pack_send.at[step, 0, part], inner_recv.at[step, places[s]])
        west = rows_of(west_send, west_recv, 0, right, tile_up(sum(WEST[:fields])))
        east = rows_of(east_send, east_recv, int(step == 0), left, tile_up(sum(EAST[:fields])))
        west.append(send(*inner(0, tail), 0, right, other))
        east.append(send(*inner(2, start), 0, left, other))
        across = send(*inner(1, whole), 0, z, other)
        folds = []
        for s, part, zz in ((2, start, mirror_w), (1, whole, mirror), (0, tail, mirror_e)):
            src, dst = pack_send.at[step, 1, part], fold_recv.at[step, places[s]]
            near = pltpu.make_async_copy(src, dst, recv_sem.at[step])
            folds.append((send(src, dst, 2 + s, zz, m), near, zz))
        return west, east, across, folds

    even = lax.rem(z, 2) == 0

    def start_all(copies):
        for copy in copies:
            copy.start()

    far_west, far_east = jnp.logical_not(even), jnp.logical_and(even, jnp.logical_not(first_z))

    def each(west_when, east_when, act, tile):
        pl.when(west_when)(lambda: act(tile[0]))
        pl.when(east_when)(lambda: act(tile[1]))

    def start_folds(folds, chosen):
        for far_copy, _, zz in folds:
            pl.when(jnp.logical_and(top, chosen(zz)))(far_copy.start)

    def take(sem, always, at_top):
        pl.when(bottom)(lambda: drain(blank.at[0:always], sem))
        pl.when(top)(lambda: drain(blank.at[0 : always + at_top], sem))

    def take_tile(step, fields):
        count = tile_up(sum(WEST[f] for f in ORDER[:fields])) + tile_up(sum(EAST[f] for f in ORDER[:fields]))
        take(recv_sem.at[step], count * ny // LANES + rows, rows)

        west = east = 0
        for f in ORDER[:fields]:
            X[f, PAD - WEST[f] : PAD, 0:ny] = west_recv[step, west : west + WEST[f], :]
            X[f, PAD + nx : PAD + nx + EAST[f], 0:ny] = east_recv[step, east : east + EAST[f], :]
            west += WEST[f]
            east += EAST[f]
        for f in range(fields):
            got = inner_recv[step]
            X[f, :, ny:width] = jnp.where(
                top, roll(got, LANES - SLOT * (f + 1), 1), roll(got, LANES - SLOT * f, 1)
            )
            G[f] = roll(fold_recv[step], LANES - SLOT * (f + 1), 1)

    pack_rows(0, 0, FIELDS - 1)
    tile = tile_0 = send_tile(0, FIELDS)
    lead = (jnp.logical_or(far_west, first_z), far_east)
    each(*lead, lambda c: c[0].start(), tile)
    loads[5].wait()
    total = thick[0]
    for l in range(1, layers):
        total = total + thick[l]
    X[5, own, 0:ny] = (WAVE_LIMIT / layers) * total
    pack_rows(0, FIELDS - 1, FIELDS)
    pack_edges(0, FIELDS)
    each(*lead, lambda c: start_all(c[1:]), tile)
    each(far_east, far_west, start_all, tile)
    tile[2].start()
    start_folds(tile[3], lambda zz: zz < z)
    for _, near_copy, zz in tile[3]:
        pl.when(jnp.logical_and(top, zz == z))(near_copy.start)

    def lay_copies(step):
        def one(src, dst, zz, mm, k=0):
            leaving[k] = leaving.get(k, 0) + lines(src)
            return pltpu.make_async_remote_copy(
                src_ref=src,
                dst_ref=dst,
                send_sem=send_sem.at[k],
                recv_sem=lay_recv_sem.at[step],
                device_id={"zonal": zz, "merid": mm},
                device_id_type=MESH,
            )

        return [
            one(lay_send_r.at[step], lay_recv_w.at[step], right, m),
            one(lay_send_l.at[step], lay_recv_e.at[step], left, m),
            one(lay_pack_send.at[step, 0], lay_pack_recv.at[step, 0], z, other),
            one(lay_pack_send.at[step, 1], lay_pack_recv.at[step, 1], mirror, m, 3),
        ]

    above = lay_send_r.shape[1] // 2

    def send_layers(step, h_ref, u_ref, v_ref):
        edge = jnp.zeros((nx, LANES), jnp.float32)
        brim = jnp.zeros((nx, LANES), jnp.float32)
        for l in range(layers):
            lay_send_r[step, l : l + 1, :] = h_ref[l, nx - 1 : nx, :]
            lay_send_r[step, above + l : above + l + 1, :] = u_ref[l, nx - 1 : nx, :]
            lay_send_l[step, l : l + 1, :] = h_ref[l, 0:1, :]
            high = roll(h_ref[l, :, last:ny], l + 1, 1)
            low = roll(h_ref[l, :, 0:LANES], l, 1)
            high_v = roll(v_ref[l, :, last:ny], layers + l + 1, 1)
            edge = jnp.where(lane == l, jnp.where(bottom, high, low), edge)
            edge = jnp.where(lane == layers + l, high_v, edge)
            brim = jnp.where(lane == l, high, brim)
        lay_pack_send[step, 0] = edge
        lay_pack_send[step, 2] = brim
        for r in range(nx):
            lay_pack_send[step, 1, r : r + 1, :] = lay_pack_send[step, 2, nx - 1 - r : nx - r, :]
        return lay_copies(step)

    def start_layers(out, first):
        out[2].start()
        late_left, late_fold = (first_z, mirror > z) if first else (False, False)
        pl.when(jnp.logical_and(top, jnp.logical_not(late_fold)))(out[3].start)
        pl.when(far_west)(lambda: start_all(out[:2]))
        pl.when(jnp.logical_and(even, jnp.logical_not(late_left)))(lambda: start_all(out[1::-1]))
        if first:
            pl.when(first_z)(out[0].start)

    def wait_layers(step):
        take(lay_recv_sem.at[step], lines(lay_recv_w.at[step]) + lines(lay_recv_e.at[step]) + nx, nx)

    def wait_sent():
        drain(blank.at[0 : leaving[0]], send_sem.at[0])
        pl.when(jnp.logical_not(first_z))(tile_0[1][0].wait_send)
        for k, zz in zip((4, 3, 2), mirrors):
            pl.when(jnp.logical_and(top, zz != z))(lambda k=k: drain(blank.at[0 : leaving[k]], send_sem.at[k]))

    drain(vel, load_sem.at[2])
    for load in loads[8:]:
        load.wait()
    out = send_layers(0, thick, vel_u, vel_v)

    start_layers(out, True)
    first = (z * nx - PAD).astype(jnp.float32)
    col = first + iota((rows, 1), 0).astype(jnp.float32) + float(total_x)
    far_col = float(2 * total_x - 1) - (first + iota((rows, 1), 0).astype(jnp.float32))
    spot = iota((1, width), 1)
    row = spot + m * ny
    row = jnp.where(jnp.logical_and(top, spot >= ny), row - width, row).astype(jnp.float32)
    far_row = (iota((1, LANES), 1) + (total_y - LANES)).astype(jnp.float32)
    px = jnp.zeros((rows, width), jnp.float32)
    py = jnp.zeros((rows, width), jnp.float32)
    fx = jnp.zeros((rows, LANES), jnp.float32)
    fy = jnp.zeros((rows, LANES), jnp.float32)
    for k in range(seeds.shape[1]):
        seed_x = seeds[0, k].astype(jnp.float32)
        seed_y = seeds[1, k].astype(jnp.float32)
        ca, sa = turns(seed_x, col, total_x)
        cf, sf = turns(seed_x, far_col, total_x)
        cb, sb = turns(seed_y, row, total_y)
        cg, sg = turns(seed_y, far_row, total_y)
        amp = scale[k]
        ca, sa, cf, sf = amp * ca, amp * sa, amp * cf, amp * sf
        px = px + (ca * cb - sa * sb)
        py = py + (sa * cb + ca * sb)
        fx = fx + (cf * cg - sf * sg)
        fy = fy + (sf * cg + cf * sg)
    wind_own[0] = px
    wind_own[1] = py
    wind_far[0] = fx
    wind_far[1] = fy

    layer_trial(thick, vel_u, vel_v, mid_h, mid_u, mid_v, sums, True)

    @pl.when(first_z)
    def _():
        pl.semaphore_wait(late_sem.at[0], 2)
        start_all(tile[1])


    @pl.when(jnp.logical_and(top, upper > 0))
    def _():
        pl.semaphore_wait(late_sem.at[1], upper)

    start_folds(tile[3], lambda zz: zz > z)
    pl.when(jnp.logical_and(top, mirror > z))(out[3].start)

    @pl.when(first_z)
    def _():
        tile[1][0].wait_send()
        out[1].start()

    take_tile(0, FIELDS)
    for k in range(2):
        X[6 + k] = STRESS_SCALE * (X[6 + k] + wind_own[k])
        G[6 + k] = STRESS_SCALE * (G[6 + k] + wind_far[k])

    lanes = iota((rows, width), 1)
    wall = jnp.logical_and(bottom, lanes == 0)
    crown = jnp.logical_and(top, lanes == ny - 1)
    far_top = iota((rows, LANES), 1) == LANES - 1

    def close_step(step, h_ref, v_ref, n_h, n_u, n_v):
        layer_edges(
            h_ref, v_ref, lay_send_r.at[step], lay_send_l.at[step], lay_recv_w.at[step], lay_recv_e.at[step],
            lay_pack_recv.at[step], n_h, n_u, n_v, sums, top, step == 0,
        )
        layer_close(n_u, n_v, sums, mean, masks, depth, step == 0)

    def substep(carry):
        eta, bu, bv, south_v, g_eta, g_bu, g_bv, g_south_v = carry
        eta = eta - (bu - roll(bu, 1, 0) + bv - south_v)
        g_eta = g_eta - (g_bu - roll(g_bu, -1, 0) + g_bv - g_south_v)
        north, south = roll(eta, -1, 1), roll(eta, 1, 1)
        north = jnp.where(crown, g_eta[:, LANES - 1 :], north)
        g_north = jnp.where(far_top, eta[:, ny - 1 : ny], roll(g_eta, -1, 1))
        g_south = roll(g_eta, 1, 1)
        bu = X[3] * (bu - X[5] * (roll(eta, -1, 0) - eta) + X[6])
        bv = X[4] * (bv - X[5] * (north - eta) + X[7])
        south_v = jnp.where(wall, 0.0, D[0] * (south_v - D[1] * (eta - south) + D[2]))
        g_bu = G[3] * (g_bu - G[5] * (roll(g_eta, 1, 0) - g_eta) + G[6])
        g_bv = G[4] * (g_bv - G[5] * (g_north - g_eta) + G[7])
        g_south_v = F[0] * (g_south_v - F[1] * (g_eta - g_south) + F[2])
        mean[0] = mean[0] + bu[own, 0:ny]
        mean[1] = mean[1] + bv[own, 0:ny]
        return eta, bu, bv, south_v, g_eta, g_bu, g_bv, g_south_v

    def substeps():
        mean[...] = jnp.zeros((2, nx, ny), jnp.float32)
        bv, g_bv = X[2], G[2]
        carry = X[0], X[1], bv, jnp.where(wall, 0.0, roll(bv, 1, 1)), G[0], G[1], g_bv, roll(g_bv, 1, 1)
        for _ in range(NSUB):
            carry = substep(carry)
        for k in range(3):
            X[k] = carry[k]
            G[k] = carry[4 + k]

    for k, f in enumerate((4, 5, 7)):
        D[k] = roll(X[f], 1, 1)
        F[k] = roll(G[f], 1, 1)
    masks = X[3, own, 0:ny], X[4, own, 0:ny]
    h_ref, u_ref, v_ref = thick, vel_u, vel_v
    n_h, n_u, n_v = mid_h, mid_u, mid_v
    for step in range(STEPS - 1):
        substeps()
        pack_rows(step + 1, 0, 3)
        tile = send_tile(step + 1, 3)
        lead = (far_west, even)
        each(*lead, lambda c: start_all(c[:-1]), tile)

        def inner_ready():
            each(*lead, lambda c: c[-1].start(), tile)
            tile[2].start()

        pack_edges(step + 1, 3, inner_ready)
        start_folds(tile[3], lambda zz: zz != z)
        for _, near_copy, zz in tile[3]:
            pl.when(jnp.logical_and(top, zz == z))(near_copy.start)
        each(even, far_west, start_all, tile)
        wait_layers(step)
        close_step(step, h_ref, v_ref, n_h, n_u, n_v)
        h_ref, u_ref, v_ref = n_h, n_u, n_v
        n_h, n_u, n_v = o_h, o_u, o_v
        out = send_layers(step + 1, h_ref, u_ref, v_ref)
        start_layers(out, False)
        layer_trial(h_ref, u_ref, v_ref, n_h, n_u, n_v, sums, False)
        take_tile(step + 1, 3)
    substeps()
    for f in range(3):
        flat[f] = X[f, own, 0:ny]
    wait_layers(STEPS - 1)
    close_step(STEPS - 1, h_ref, v_ref, n_h, n_u, n_v)
    wait_sent()


def body(zonal_devices, merid_devices, *args):
    thickness = args[3]
    layers, nx, ny = thickness.shape
    up = tile_up(layers)
    f32 = jnp.float32
    vmem = pl.BlockSpec(memory_space=pltpu.VMEM)
    far = pl.BlockSpec(memory_space=pltpu.HBM)
    hbm = pl.BlockSpec(memory_space=pl.ANY)
    rows = nx + 2 * PAD
    west, east = tile_up(sum(WEST)), tile_up(sum(EAST))
    plane = jax.ShapeDtypeStruct((nx, ny), f32)
    solid = jax.ShapeDtypeStruct((layers, nx, ny), f32)
    kept = [(3, nx, ny), (layers, nx, ny), (layers, nx, ny), (layers, nx, ny)]
    room = sum(math.prod(shape) for shape in kept)
    args = list(args)
    args[7] = args[7].T
    between = pl.pallas_call(
        functools.partial(kernel, zonal_devices, merid_devices),
        out_shape=[pltpu.VMEM(shape, f32) for shape in kept],
        in_specs=[far] * 10,
        out_specs=[vmem] * len(kept),
        scratch_shapes=[
            pltpu.VMEM((layers, nx, ny), f32),
            pltpu.VMEM((2, layers, nx, ny), f32),
            pltpu.VMEM((2, nx, ny), jnp.int32),
            pltpu.SMEM(args[7].shape, jnp.int32),
            pltpu.SMEM(args[8].shape, f32),
            pltpu.VMEM((layers, nx, ny), f32),
            pltpu.VMEM((layers, nx, ny), f32),
            pltpu.VMEM((layers, nx, ny), f32),
            pltpu.VMEM((2, nx, ny), f32),
            pltpu.VMEM((4, nx, ny), f32),
            pltpu.VMEM((2, nx, ny), f32),
            pltpu.VMEM((FIELDS, rows, ny + LANES), f32),
            pltpu.VMEM((FIELDS, rows, LANES), f32),
            pltpu.VMEM((3, rows, ny + LANES), f32),
            pltpu.VMEM((3, rows, LANES), f32),
            pltpu.VMEM((2, rows, ny + LANES), f32),
            pltpu.VMEM((2, rows, LANES), f32),
            pltpu.VMEM((STEPS, west, ny), f32),
            pltpu.VMEM((STEPS, west, ny), f32),
            pltpu.VMEM((STEPS, east, ny), f32),
            pltpu.VMEM((STEPS, east, ny), f32),
            pltpu.VMEM((STEPS, 3, nx, LANES), f32),
            pltpu.VMEM((STEPS, rows, LANES), f32),
            pltpu.VMEM((STEPS, rows, LANES), f32),
            pltpu.VMEM((STEPS, 2 * up, ny), f32),
            pltpu.VMEM((STEPS, up, ny), f32),
            pltpu.VMEM((STEPS, 2 * up, ny), f32),
            pltpu.VMEM((STEPS, up, ny), f32),
            pltpu.VMEM((STEPS, 3, nx, LANES), f32),
            pltpu.VMEM((STEPS, 2, nx, LANES), f32),
            pltpu.VMEM((4 * (west + east) * ny // LANES, LANES), f32),
            pltpu.SemaphoreType.DMA((5,)),
            pltpu.SemaphoreType.DMA((5,)),
            pltpu.SemaphoreType.DMA((STEPS,)),
            pltpu.SemaphoreType.DMA((STEPS,)),
            pltpu.SemaphoreType.REGULAR((2,)),
        ],
        compiler_params=pltpu.CompilerParams(
            collective_id=0, has_side_effects=True, vmem_limit_bytes=VMEM_BYTES - 4 * room - SPARE
        ),
        name="ocean",
    )(*args)
    return pl.pallas_call(
        last_kernel,
        out_shape=(plane, plane, plane, solid, solid, solid),
        in_specs=[vmem] * len(kept),
        out_specs=[hbm] * 6,
        scratch_shapes=[pltpu.SemaphoreType.DMA((4,))],
        compiler_params=pltpu.CompilerParams(vmem_limit_bytes=24 * 1024 * 1024),
        name="last",
    )(*between)


def solution(mesh):
    field = P(("members", "zonal"), "merid")
    solid = P(None, ("members", "zonal"), "merid")
    fixed = P(None, "zonal", "merid")
    return jax.shard_map(
        functools.partial(body, mesh.shape["zonal"], mesh.shape["merid"]),
        mesh=mesh,
        in_specs=(
            field, field, field, solid, solid, solid, fixed, P("members", None), P("members"), fixed,
        ),
        out_specs=(field, field, field, solid, solid, solid),
        check_vma=False,
    )
```

```python
import functools
import math

import jax
import jax.numpy as jnp
from jax import lax
from jax.experimental import pallas as pl
from jax.experimental.pallas import tpu as pltpu
from jax.sharding import PartitionSpec as P

NSUB = 6
STEPS = 2
MARGIN = NSUB
PAD = 8

WAVE_LIMIT = 0.225
STRESS_SCALE = 0.1
FLUX_STEP = 0.05
PRESS_COEF = 0.05
LANES = 128
VMEM_BYTES = 67043328
SPARE = 1 << 15
FIELDS = 8
SLOT = LANES // FIELDS
WEST = (NSUB - 1, NSUB, NSUB - 1, NSUB - 1, NSUB - 2, NSUB - 1, NSUB - 1, NSUB - 2)
EAST = (NSUB, NSUB, NSUB) + (NSUB - 1,) * 5
ORDER = (0, 1, 2, 3, 4, 6, 7, 5)
CUT = 32
MESH = pl.DeviceIdType.MESH


def roll(value, shift, axis):
    return pltpu.roll(value, shift % value.shape[axis], axis)


def iota(shape, axis):
    return lax.broadcasted_iota(jnp.int32, shape, axis)


def turns(seed, index, total):
    part = seed * index * (1.0 / total)
    angle = (2.0 * math.pi) * (part - jnp.floor(part))
    return jnp.cos(angle), jnp.sin(angle)


def lines(ref):
    return math.prod(ref.shape) // LANES


def drain(ref, sem):
    pltpu.make_async_copy(ref, ref, sem).wait()


def tile_up(count):
    return -(-count // 8) * 8


def layer_trial(h_ref, u_ref, v_ref, o_h, o_u, o_v, sums, deep):
    layers, nx, ny = h_ref.shape
    at_east = iota((nx, ny), 0) == nx - 1
    at_north = iota((nx, ny), 1) == ny - 1
    zero = jnp.zeros((nx, ny), jnp.float32)
    press_u, press_v, sum_u, sum_v = zero, zero, zero, zero
    deep_u, deep_v = zero, zero
    for l in range(layers):
        h, u, v = h_ref[l], u_ref[l], v_ref[l]
        h_east, h_north = roll(h, -1, 0), roll(h, -1, 1)
        hu = (h + h_east) * 0.5
        hv = (h + h_north) * 0.5
        if deep:
            deep_u = deep_u + hu
            deep_v = deep_v + hv
        flux_u = jnp.where(at_east, 0.0, u * hu)
        flux_v = jnp.where(at_north, 0.0, v * hv)
        press_u = press_u + (h_east - h)
        press_v = press_v + (h_north - h)
        trial_u = u - PRESS_COEF * press_u
        trial_v = v - PRESS_COEF * press_v
        sum_u = sum_u + hu * trial_u
        sum_v = sum_v + hv * trial_v
        o_u[l] = trial_u
        o_v[l] = trial_v
        o_h[l] = h - FLUX_STEP * (flux_u - roll(flux_u, 1, 0) + flux_v - roll(flux_v, 1, 1))
    sums[0] = sum_u
    sums[1] = sum_v
    if deep:
        sums[2] = deep_u
        sums[3] = deep_v


def layer_edges(h_ref, v_ref, own_r, own_l, recv_w, recv_e, packs, o_h, o_u, o_v, sums, top, deep):
    layers, nx, ny = h_ref.shape
    up = own_l.shape[0]
    layer = iota((up, ny), 0)
    h_last, u_last, h_first = own_r[0:up], own_r[up:], own_l[...]
    h_e, h_w, u_w = recv_e[...], recv_w[0:up], recv_w[up:]
    hu = (h_last + h_e) * 0.5
    press = h_e - h_last
    step = 1
    while step < layers:
        press = press + jnp.where(layer >= step, roll(press, step, 0), 0.0)
        step *= 2
    trial = u_last - PRESS_COEF * press
    outflow = FLUX_STEP * (u_last * hu)
    inflow = FLUX_STEP * (u_w * ((h_w + h_first) * 0.5))
    whole = lambda a: jnp.sum(jnp.where(layer < layers, a, 0.0), axis=0, keepdims=True)
    sums[0, nx - 1 : nx, :] = whole(hu * trial)
    if deep:
        sums[2, nx - 1 : nx, :] = whole(hu)
    for l in range(layers):
        o_u[l, nx - 1 : nx, :] = trial[l : l + 1]
        o_h[l, nx - 1 : nx, :] = o_h[l, nx - 1 : nx, :] - outflow[l : l + 1]
        o_h[l, 0:1, :] = o_h[l, 0:1, :] + inflow[l : l + 1]

    lane = iota((nx, LANES), 1)
    last = ny - LANES
    at_end = lane == LANES - 1
    at_start = jnp.logical_and(top, lane == 0)
    side = packs[0]
    cap = jnp.where(top, packs[1], side)
    press, total, deep_v = 0.0, 0.0, 0.0
    for l in range(layers):
        h, v = h_ref[l, :, last:ny], v_ref[l, :, last:ny]
        h_north = roll(cap, LANES - 1 - l, 1)
        hv = (h + h_north) * 0.5
        press = press + (h_north - h)
        trial = v - PRESS_COEF * press
        total = total + hv * trial
        deep_v = deep_v + hv
        o_v[l, :, last:ny] = jnp.where(at_end, trial, o_v[l, :, last:ny])
        o_h[l, :, last:ny] = o_h[l, :, last:ny] - jnp.where(at_end, FLUX_STEP * (v * hv), 0.0)
        h_south, v_south = roll(side, -l, 1), roll(side, -(layers + l), 1)
        inflow = FLUX_STEP * (v_south * ((h_south + h_ref[l, :, 0:LANES]) * 0.5))
        o_h[l, :, 0:LANES] = o_h[l, :, 0:LANES] + jnp.where(at_start, inflow, 0.0)
    sums[1, :, last:ny] = jnp.where(at_end, total, sums[1, :, last:ny])
    if deep:
        sums[3, :, last:ny] = jnp.where(at_end, deep_v, sums[3, :, last:ny])


def layer_close(o_u, o_v, sums, mean, masks, depth, deep):
    if deep:
        depth[0] = 1.0 / sums[2]
        depth[1] = 1.0 / sums[3]
    for k, out in enumerate((o_u, o_v)):
        fix = (mean[k] * (1.0 / NSUB) - sums[k]) * depth[k]
        mask = masks[k]
        for l in range(out.shape[0]):
            out[l] = mask * (out[l] + fix)


def last_kernel(flat, n_h, n_u, n_v, o_eta, o_bu, o_bv, o_h, o_u, o_v, sems):
    moves = [(flat.at[k], o, 0) for k, o in enumerate((o_eta, o_bu, o_bv))]
    moves += [(n_h, o_h, 1), (n_u, o_u, 2), (n_v, o_v, 3)]
    copies = [pltpu.make_async_copy(src, dst, sems.at[k]) for src, dst, k in moves]
    for copy in copies:
        copy.start()
    drain(flat, sems.at[0])
    for copy in copies[3:]:
        copy.wait()


def kernel(
    zonal_devices,
    merid_devices,
    height_any,
    trans_u_any,
    trans_v_any,
    thick_any,
    vel_u_any,
    vel_v_any,
    faces_any,
    seeds_any,
    scale_any,
    base_any,
    flat,
    o_h,
    o_u,
    o_v,
    thick,
    vel,
    faces,
    seeds,
    scale,
    mid_h,
    mid_u,
    mid_v,
    mean,
    sums,
    depth,
    X,
    G,
    D,
    F,
    wind_own,
    wind_far,
    west_send,
    west_recv,
    east_send,
    east_recv,
    pack_send,
    inner_recv,
    fold_recv,
    lay_send_r,
    lay_send_l,
    lay_recv_w,
    lay_recv_e,
    lay_pack_send,
    lay_pack_recv,
    blank,
    load_sem,
    send_sem,
    recv_sem,
    lay_recv_sem,
    late_sem,
):
    layers, nx, ny = thick.shape
    Z = zonal_devices
    total_x, total_y = nx * Z, ny * merid_devices
    z = lax.axis_index("zonal")
    m = lax.axis_index("merid")
    other = 1 - m
    bottom = m == 0
    top = m == merid_devices - 1
    right, left = lax.rem(z + 1, Z), lax.rem(z + Z - 1, Z)
    mirror = Z - 1 - z
    mirror_e, mirror_w = lax.rem(mirror + 1, Z), lax.rem(mirror + Z - 1, Z)
    rows = nx + 2 * PAD
    width = ny + LANES
    last = ny - LANES
    own = slice(PAD, PAD + nx)
    lane = iota((nx, LANES), 1)

    barrier = pltpu.get_barrier_semaphore()
    first_z, last_z = z == 0, z == Z - 1
    late_left = jnp.logical_or(first_z, last_z)
    mirrors = (mirror_w, mirror, mirror_e)

    def greet(sem, zz, mm):
        pl.semaphore_signal(sem, inc=1, device_id={"zonal": zz, "merid": mm}, device_id_type=MESH)

    greet(barrier, z, other)
    for mm in (m, other):
        greet(barrier, left, mm)
        pl.when(z < Z - 2)(lambda mm=mm: greet(barrier, right, mm))

    for zz in mirrors:

        @pl.when(jnp.logical_and(top, zz > z))
        def _():
            greet(barrier, zz, m)

    moves = (
        (faces_any, faces),
        (height_any, X.at[0, own, 0:ny]),
        (trans_u_any, X.at[1, own, 0:ny]),
        (trans_v_any, X.at[2, own, 0:ny]),
        (base_any, X.at[6:8, own, 0:ny]),
        (thick_any, thick),
        (vel_u_any, vel.at[0]),
        (vel_v_any, vel.at[1]),
        (seeds_any, seeds),
        (scale_any, scale),
    )
    group = (0, 0, 0, 0, 0, 1, 2, 2, 3, 4)
    vel_u, vel_v = vel.at[0], vel.at[1]
    loads = [pltpu.make_async_copy(src, dst, load_sem.at[k]) for k, (src, dst) in zip(group, moves)]
    for load in loads:
        load.start()

    near = 3 + jnp.where(jnp.logical_or(first_z, last_z), 0, 2)
    lower = sum((zz < z).astype(jnp.int32) for zz in mirrors)
    upper = sum((zz > z).astype(jnp.int32) for zz in mirrors)
    pl.semaphore_wait(barrier, near + jnp.where(top, lower, 0))

    @pl.when(z >= Z - 2)
    def _():
        for mm in (m, other):
            greet(late_sem.at[0], right, mm)

    for zz in mirrors:

        @pl.when(jnp.logical_and(top, zz < z))
        def _():
            greet(late_sem.at[1], zz, m)

    drain(blank.at[0 : sum(lines(dst) for _, dst in moves[:5])], load_sem.at[0])
    X[3, own, 0:ny] = faces[0].astype(jnp.float32)
    X[4, own, 0:ny] = faces[1].astype(jnp.float32)

    def pack_rows(step, start, stop):
        west = sum(WEST[f] for f in ORDER[:start])
        east = sum(EAST[f] for f in ORDER[:start])
        for f in ORDER[start:stop]:
            west_send[step, west : west + WEST[f], :] = X[f, PAD + nx - WEST[f] : PAD + nx, 0:ny]
            east_send[step, east : east + EAST[f], :] = X[f, PAD : PAD + EAST[f], 0:ny]
            west += WEST[f]
            east += EAST[f]

    def pack_edges(step, fields, between=lambda: None):
        inner = jnp.zeros((nx, LANES), jnp.float32)
        crest = jnp.zeros((nx, LANES), jnp.float32)
        for f in range(fields):
            here = jnp.logical_and(lane >= f * SLOT, lane < (f + 1) * SLOT)
            high = roll(X[f, own, last:ny], SLOT * (f + 1), 1)
            low = roll(X[f, own, 0:LANES], SLOT * f, 1)
            crest = jnp.where(here, high, crest)
            inner = jnp.where(here, jnp.where(bottom, high, low), inner)
        pack_send[step, 0] = inner
        between()
        pack_send[step, 2] = crest
        for r in range(nx):
            pack_send[step, 1, r : r + 1, :] = pack_send[step, 2, nx - 1 - r : nx - r, :]

    leaving = {}

    def send_tile(step, fields):
        def send(src, dst, k, zz, mm):
            leaving[k] = leaving.get(k, 0) + lines(src)
            return pltpu.make_async_remote_copy(
                src_ref=src,
                dst_ref=dst,
                send_sem=send_sem.at[k],
                recv_sem=recv_sem.at[step],
                device_id={"zonal": zz, "merid": mm},
                device_id_type=MESH,
            )

        def rows_of(src, dst, k, zz, count):
            cuts = [0, CUT, count] if count > CUT else [0, count]
            parts = [slice(low, high) for low, high in zip(cuts[:-1], cuts[1:])]
            return [send(src.at[step, p], dst.at[step, p], k, zz, m) for p in parts]

        tail, whole, start = slice(nx - PAD, nx), slice(0, nx), slice(0, PAD)
        places = (slice(0, PAD), own, slice(PAD + nx, rows))
        inner = lambda s, part: (pack_send.at[step, 0, part], inner_recv.at[step, places[s]])
        west = rows_of(west_send, west_recv, 0, right, tile_up(sum(WEST[:fields])))
        east = rows_of(east_send, east_recv, int(step == 0), left, tile_up(sum(EAST[:fields])))
        west.append(send(*inner(0, tail), 0, right, other))
        east.append(send(*inner(2, start), int(step == 0), left, other))
        across = send(*inner(1, whole), 0, z, other)
        folds = []
        for s, part, zz in ((2, start, mirror_w), (1, whole, mirror), (0, tail, mirror_e)):
            src, dst = pack_send.at[step, 1, part], fold_recv.at[step, places[s]]
            near = pltpu.make_async_copy(src, dst, recv_sem.at[step])
            folds.append((send(src, dst, 2 + s, zz, m), near, zz))
        return west, east, across, folds

    even = lax.rem(z, 2) == 0

    def start_all(copies):
        for copy in copies:
            copy.start()

    far_west, far_east = jnp.logical_not(even), jnp.logical_and(even, jnp.logical_not(first_z))

    def each(west_when, east_when, act, tile):
        pl.when(west_when)(lambda: act(tile[0]))
        pl.when(east_when)(lambda: act(tile[1]))

    def start_folds(folds, chosen):
        for far_copy, _, zz in folds:
            pl.when(jnp.logical_and(top, chosen(zz)))(far_copy.start)

    def take(sem, always, at_top):
        pl.when(bottom)(lambda: drain(blank.at[0:always], sem))
        pl.when(top)(lambda: drain(blank.at[0 : always + at_top], sem))

    def take_tile(step, fields):
        count = tile_up(sum(WEST[f] for f in ORDER[:fields])) + tile_up(sum(EAST[f] for f in ORDER[:fields]))
        take(recv_sem.at[step], count * ny // LANES + rows, rows)

        west = east = 0
        for f in ORDER[:fields]:
            X[f, PAD - WEST[f] : PAD, 0:ny] = west_recv[step, west : west + WEST[f], :]
            X[f, PAD + nx : PAD + nx + EAST[f], 0:ny] = east_recv[step, east : east + EAST[f], :]
            west += WEST[f]
            east += EAST[f]
        for f in range(fields):
            got = inner_recv[step]
            X[f, :, ny:width] = jnp.where(
                top, roll(got, LANES - SLOT * (f + 1), 1), roll(got, LANES - SLOT * f, 1)
            )
            G[f] = roll(fold_recv[step], LANES - SLOT * (f + 1), 1)

    pack_rows(0, 0, FIELDS - 1)
    tile = tile_0 = send_tile(0, FIELDS)
    lead = (jnp.logical_or(far_west, first_z), far_east)
    each(*lead, lambda c: c[0].start(), tile)
    loads[5].wait()
    total = thick[0]
    for l in range(1, layers):
        total = total + thick[l]
    X[5, own, 0:ny] = (WAVE_LIMIT / layers) * total
    pack_rows(0, FIELDS - 1, FIELDS)
    pack_edges(0, FIELDS)
    each(*lead, lambda c: start_all(c[1:]), tile)
    each(far_east, jnp.logical_and(far_west, jnp.logical_not(last_z)), start_all, tile)
    tile[2].start()
    start_folds(tile[3], lambda zz: zz < z)
    for _, near_copy, zz in tile[3]:
        pl.when(jnp.logical_and(top, zz == z))(near_copy.start)

    def lay_copies(step):
        def one(src, dst, zz, mm, k=0):
            leaving[k] = leaving.get(k, 0) + lines(src)
            return pltpu.make_async_remote_copy(
                src_ref=src,
                dst_ref=dst,
                send_sem=send_sem.at[k],
                recv_sem=lay_recv_sem.at[step],
                device_id={"zonal": zz, "merid": mm},
                device_id_type=MESH,
            )

        return [
            one(lay_send_r.at[step], lay_recv_w.at[step], right, m),
            one(lay_send_l.at[step], lay_recv_e.at[step], left, m),
            one(lay_pack_send.at[step, 0], lay_pack_recv.at[step, 0], z, other),
            one(lay_pack_send.at[step, 1], lay_pack_recv.at[step, 1], mirror, m, 3),
        ]

    above = lay_send_r.shape[1] // 2

    def send_layers(step, h_ref, u_ref, v_ref):
        edge = jnp.zeros((nx, LANES), jnp.float32)
        brim = jnp.zeros((nx, LANES), jnp.float32)
        for l in range(layers):
            lay_send_r[step, l : l + 1, :] = h_ref[l, nx - 1 : nx, :]
            lay_send_r[step, above + l : above + l + 1, :] = u_ref[l, nx - 1 : nx, :]
            lay_send_l[step, l : l + 1, :] = h_ref[l, 0:1, :]
            high = roll(h_ref[l, :, last:ny], l + 1, 1)
            low = roll(h_ref[l, :, 0:LANES], l, 1)
            high_v = roll(v_ref[l, :, last:ny], layers + l + 1, 1)
            edge = jnp.where(lane == l, jnp.where(bottom, high, low), edge)
            edge = jnp.where(lane == layers + l, high_v, edge)
            brim = jnp.where(lane == l, high, brim)
        lay_pack_send[step, 0] = edge
        lay_pack_send[step, 2] = brim
        for r in range(nx):
            lay_pack_send[step, 1, r : r + 1, :] = lay_pack_send[step, 2, nx - 1 - r : nx - r, :]
        return lay_copies(step)

    def start_layers(out, first):
        out[2].start()
        hold, late_fold = (late_left, mirror > z) if first else (False, False)
        pl.when(jnp.logical_and(top, jnp.logical_not(late_fold)))(out[3].start)
        pl.when(far_west)(out[0].start)
        pl.when(jnp.logical_not(hold))(out[1].start)
        pl.when(jnp.logical_not(far_west))(out[0].start)

    def wait_layers(step):
        take(lay_recv_sem.at[step], lines(lay_recv_w.at[step]) + lines(lay_recv_e.at[step]) + nx, nx)

    def wait_sent():
        drain(blank.at[0 : leaving[0]], send_sem.at[0])
        pl.when(jnp.logical_not(first_z))(lambda: drain(blank.at[0 : leaving[1]], send_sem.at[1]))
        for k, zz in zip((4, 3, 2), mirrors):
            pl.when(jnp.logical_and(top, zz != z))(lambda k=k: drain(blank.at[0 : leaving[k]], send_sem.at[k]))

    drain(vel, load_sem.at[2])
    for load in loads[8:]:
        load.wait()
    out = send_layers(0, thick, vel_u, vel_v)

    start_layers(out, True)
    first = (z * nx - PAD).astype(jnp.float32)
    col = first + iota((rows, 1), 0).astype(jnp.float32) + float(total_x)
    far_col = float(2 * total_x - 1) - (first + iota((rows, 1), 0).astype(jnp.float32))
    spot = iota((1, width), 1)
    row = spot + m * ny
    row = jnp.where(jnp.logical_and(top, spot >= ny), row - width, row).astype(jnp.float32)
    far_row = (iota((1, LANES), 1) + (total_y - LANES)).astype(jnp.float32)
    px = jnp.zeros((rows, width), jnp.float32)
    py = jnp.zeros((rows, width), jnp.float32)
    fx = jnp.zeros((rows, LANES), jnp.float32)
    fy = jnp.zeros((rows, LANES), jnp.float32)
    for k in range(seeds.shape[1]):
        seed_x = seeds[0, k].astype(jnp.float32)
        seed_y = seeds[1, k].astype(jnp.float32)
        ca, sa = turns(seed_x, col, total_x)
        cf, sf = turns(seed_x, far_col, total_x)
        cb, sb = turns(seed_y, row, total_y)
        cg, sg = turns(seed_y, far_row, total_y)
        amp = scale[k]
        ca, sa, cf, sf = amp * ca, amp * sa, amp * cf, amp * sf
        px = px + (ca * cb - sa * sb)
        py = py + (sa * cb + ca * sb)
        fx = fx + (cf * cg - sf * sg)
        fy = fy + (sf * cg + cf * sg)
    wind_own[0] = px
    wind_own[1] = py
    wind_far[0] = fx
    wind_far[1] = fy

    layer_trial(thick, vel_u, vel_v, mid_h, mid_u, mid_v, sums, True)

    @pl.when(late_left)
    def _():
        pl.semaphore_wait(late_sem.at[0], 2)
        start_all(tile[1])


    @pl.when(jnp.logical_and(top, upper > 0))
    def _():
        pl.semaphore_wait(late_sem.at[1], upper)

    start_folds(tile[3], lambda zz: zz > z)
    pl.when(jnp.logical_and(top, mirror > z))(out[3].start)

    @pl.when(first_z)
    def _():
        drain(blank.at[0 : leaving[1]], send_sem.at[1])

    pl.when(late_left)(out[1].start)

    take_tile(0, FIELDS)
    for k in range(2):
        X[6 + k] = STRESS_SCALE * (X[6 + k] + wind_own[k])
        G[6 + k] = STRESS_SCALE * (G[6 + k] + wind_far[k])

    lanes = iota((rows, width), 1)
    wall = jnp.logical_and(bottom, lanes == 0)
    crown = jnp.logical_and(top, lanes == ny - 1)
    far_top = iota((rows, LANES), 1) == LANES - 1

    def close_step(step, h_ref, v_ref, n_h, n_u, n_v):
        layer_edges(
            h_ref, v_ref, lay_send_r.at[step], lay_send_l.at[step], lay_recv_w.at[step], lay_recv_e.at[step],
            lay_pack_recv.at[step], n_h, n_u, n_v, sums, top, step == 0,
        )
        layer_close(n_u, n_v, sums, mean, masks, depth, step == 0)

    def substep(carry):
        eta, bu, bv, south_v, g_eta, g_bu, g_bv, g_south_v = carry
        eta = eta - (bu - roll(bu, 1, 0) + bv - south_v)
        g_eta = g_eta - (g_bu - roll(g_bu, -1, 0) + g_bv - g_south_v)
        north, south = roll(eta, -1, 1), roll(eta, 1, 1)
        north = jnp.where(crown, g_eta[:, LANES - 1 :], north)
        g_north = jnp.where(far_top, eta[:, ny - 1 : ny], roll(g_eta, -1, 1))
        g_south = roll(g_eta, 1, 1)
        bu = X[3] * (bu - X[5] * (roll(eta, -1, 0) - eta) + X[6])
        bv = X[4] * (bv - X[5] * (north - eta) + X[7])
        south_v = jnp.where(wall, 0.0, D[0] * (south_v - D[1] * (eta - south) + D[2]))
        g_bu = G[3] * (g_bu - G[5] * (roll(g_eta, 1, 0) - g_eta) + G[6])
        g_bv = G[4] * (g_bv - G[5] * (g_north - g_eta) + G[7])
        g_south_v = F[0] * (g_south_v - F[1] * (g_eta - g_south) + F[2])
        mean[0] = mean[0] + bu[own, 0:ny]
        mean[1] = mean[1] + bv[own, 0:ny]
        return eta, bu, bv, south_v, g_eta, g_bu, g_bv, g_south_v

    def substeps(out):
        mean[...] = jnp.zeros((2, nx, ny), jnp.float32)
        bv, g_bv = X[2], G[2]
        carry = X[0], X[1], bv, jnp.where(wall, 0.0, roll(bv, 1, 1)), G[0], G[1], g_bv, roll(g_bv, 1, 1)
        for _ in range(NSUB):
            carry = substep(carry)
        for k in range(3):
            out[k, ...] = carry[k][own, 0:ny]

    for k, f in enumerate((4, 5, 7)):
        D[k] = roll(X[f], 1, 1)
        F[k] = roll(G[f], 1, 1)
    masks = X[3, own, 0:ny], X[4, own, 0:ny]
    h_ref, u_ref, v_ref = thick, vel_u, vel_v
    n_h, n_u, n_v = mid_h, mid_u, mid_v
    for step in range(STEPS - 1):
        substeps(X.at[0:3, own, 0:ny])
        pack_rows(step + 1, 0, 3)
        tile = send_tile(step + 1, 3)
        lead = (far_west, even)
        each(*lead, lambda c: start_all(c[:-1]), tile)

        def inner_ready():
            each(*lead, lambda c: c[-1].start(), tile)
            tile[2].start()

        pack_edges(step + 1, 3, inner_ready)
        start_folds(tile[3], lambda zz: zz != z)
        for _, near_copy, zz in tile[3]:
            pl.when(jnp.logical_and(top, zz == z))(near_copy.start)
        each(even, far_west, start_all, tile)
        wait_layers(step)
        close_step(step, h_ref, v_ref, n_h, n_u, n_v)
        h_ref, u_ref, v_ref = n_h, n_u, n_v
        n_h, n_u, n_v = o_h, o_u, o_v
        out = send_layers(step + 1, h_ref, u_ref, v_ref)
        start_layers(out, False)
        layer_trial(h_ref, u_ref, v_ref, n_h, n_u, n_v, sums, False)
        take_tile(step + 1, 3)
    substeps(flat)
    wait_layers(STEPS - 1)
    close_step(STEPS - 1, h_ref, v_ref, n_h, n_u, n_v)
    wait_sent()


def body(zonal_devices, merid_devices, *args):
    thickness = args[3]
    layers, nx, ny = thickness.shape
    up = tile_up(layers)
    f32 = jnp.float32
    vmem = pl.BlockSpec(memory_space=pltpu.VMEM)
    far = pl.BlockSpec(memory_space=pltpu.HBM)
    hbm = pl.BlockSpec(memory_space=pl.ANY)
    rows = nx + 2 * PAD
    west, east = tile_up(sum(WEST)), tile_up(sum(EAST))
    plane = jax.ShapeDtypeStruct((nx, ny), f32)
    solid = jax.ShapeDtypeStruct((layers, nx, ny), f32)
    kept = [(3, nx, ny), (layers, nx, ny), (layers, nx, ny), (layers, nx, ny)]
    room = sum(math.prod(shape) for shape in kept)
    args = list(args)
    args[7] = args[7].T
    between = pl.pallas_call(
        functools.partial(kernel, zonal_devices, merid_devices),
        out_shape=[pltpu.VMEM(shape, f32) for shape in kept],
        in_specs=[far] * 10,
        out_specs=[vmem] * len(kept),
        scratch_shapes=[
            pltpu.VMEM((layers, nx, ny), f32),
            pltpu.VMEM((2, layers, nx, ny), f32),
            pltpu.VMEM((2, nx, ny), jnp.int32),
            pltpu.SMEM(args[7].shape, jnp.int32),
            pltpu.SMEM(args[8].shape, f32),
            pltpu.VMEM((layers, nx, ny), f32),
            pltpu.VMEM((layers, nx, ny), f32),
            pltpu.VMEM((layers, nx, ny), f32),
            pltpu.VMEM((2, nx, ny), f32),
            pltpu.VMEM((4, nx, ny), f32),
            pltpu.VMEM((2, nx, ny), f32),
            pltpu.VMEM((FIELDS, rows, ny + LANES), f32),
            pltpu.VMEM((FIELDS, rows, LANES), f32),
            pltpu.VMEM((3, rows, ny + LANES), f32),
            pltpu.VMEM((3, rows, LANES), f32),
            pltpu.VMEM((2, rows, ny + LANES), f32),
            pltpu.VMEM((2, rows, LANES), f32),
            pltpu.VMEM((STEPS, west, ny), f32),
            pltpu.VMEM((STEPS, west, ny), f32),
            pltpu.VMEM((STEPS, east, ny), f32),
            pltpu.VMEM((STEPS, east, ny), f32),
            pltpu.VMEM((STEPS, 3, nx, LANES), f32),
            pltpu.VMEM((STEPS, rows, LANES), f32),
            pltpu.VMEM((STEPS, rows, LANES), f32),
            pltpu.VMEM((STEPS, 2 * up, ny), f32),
            pltpu.VMEM((STEPS, up, ny), f32),
            pltpu.VMEM((STEPS, 2 * up, ny), f32),
            pltpu.VMEM((STEPS, up, ny), f32),
            pltpu.VMEM((STEPS, 3, nx, LANES), f32),
            pltpu.VMEM((STEPS, 2, nx, LANES), f32),
            pltpu.VMEM((4 * (west + east) * ny // LANES, LANES), f32),
            pltpu.SemaphoreType.DMA((5,)),
            pltpu.SemaphoreType.DMA((5,)),
            pltpu.SemaphoreType.DMA((STEPS,)),
            pltpu.SemaphoreType.DMA((STEPS,)),
            pltpu.SemaphoreType.REGULAR((2,)),
        ],
        compiler_params=pltpu.CompilerParams(
            collective_id=0, has_side_effects=True, vmem_limit_bytes=VMEM_BYTES - 4 * room - SPARE
        ),
        name="ocean",
    )(*args)
    return pl.pallas_call(
        last_kernel,
        out_shape=(plane, plane, plane, solid, solid, solid),
        in_specs=[vmem] * len(kept),
        out_specs=[hbm] * 6,
        scratch_shapes=[pltpu.SemaphoreType.DMA((4,))],
        compiler_params=pltpu.CompilerParams(vmem_limit_bytes=24 * 1024 * 1024),
        name="last",
    )(*between)


def solution(mesh):
    field = P(("members", "zonal"), "merid")
    solid = P(None, ("members", "zonal"), "merid")
    fixed = P(None, "zonal", "merid")
    return jax.shard_map(
        functools.partial(body, mesh.shape["zonal"], mesh.shape["merid"]),
        mesh=mesh,
        in_specs=(
            field, field, field, solid, solid, solid, fixed, P("members", None), P("members"), fixed,
        ),
        out_specs=(field, field, field, solid, solid, solid),
        check_vma=False,
    )
```

```python
import functools
import math

import jax
import jax.numpy as jnp
from jax import lax
from jax.experimental import pallas as pl
from jax.experimental.pallas import tpu as pltpu
from jax.sharding import PartitionSpec as P

NSUB = 6
STEPS = 2
MARGIN = NSUB
PAD = 8

WAVE_LIMIT = 0.225
STRESS_SCALE = 0.1
FLUX_STEP = 0.05
PRESS_COEF = 0.05
LANES = 128
VMEM_BYTES = 67043328
SPARE = 1 << 15
FIELDS = 8
SLOT = LANES // FIELDS
WEST = (NSUB - 1, NSUB, NSUB - 1, NSUB - 1, NSUB - 2, NSUB - 1, NSUB - 1, NSUB - 2)
EAST = (NSUB, NSUB, NSUB) + (NSUB - 1,) * 5
ORDER = (0, 1, 2, 3, 4, 6, 7, 5)
CUT = 32
MESH = pl.DeviceIdType.MESH


def roll(value, shift, axis):
    return pltpu.roll(value, shift % value.shape[axis], axis)


def iota(shape, axis):
    return lax.broadcasted_iota(jnp.int32, shape, axis)


def turns(seed, index, total):
    part = seed * index * (1.0 / total)
    angle = (2.0 * math.pi) * (part - jnp.floor(part))
    return jnp.cos(angle), jnp.sin(angle)


def lines(ref):
    return math.prod(ref.shape) // LANES


def drain(ref, sem):
    pltpu.make_async_copy(ref, ref, sem).wait()


def tile_up(count):
    return -(-count // 8) * 8


def layer_trial(h_ref, u_ref, v_ref, o_h, o_u, o_v, sums, deep):
    layers, nx, ny = h_ref.shape
    at_east = iota((nx, ny), 0) == nx - 1
    at_north = iota((nx, ny), 1) == ny - 1
    zero = jnp.zeros((nx, ny), jnp.float32)
    press_u, press_v, sum_u, sum_v = zero, zero, zero, zero
    deep_u, deep_v = zero, zero
    for l in range(layers):
        h, u, v = h_ref[l], u_ref[l], v_ref[l]
        h_east, h_north = roll(h, -1, 0), roll(h, -1, 1)
        hu = (h + h_east) * 0.5
        hv = (h + h_north) * 0.5
        if deep:
            deep_u = deep_u + hu
            deep_v = deep_v + hv
        flux_u = jnp.where(at_east, 0.0, u * hu)
        flux_v = jnp.where(at_north, 0.0, v * hv)
        press_u = press_u + (h_east - h)
        press_v = press_v + (h_north - h)
        trial_u = u - PRESS_COEF * press_u
        trial_v = v - PRESS_COEF * press_v
        sum_u = sum_u + hu * trial_u
        sum_v = sum_v + hv * trial_v
        o_u[l] = trial_u
        o_v[l] = trial_v
        o_h[l] = h - FLUX_STEP * (flux_u - roll(flux_u, 1, 0) + flux_v - roll(flux_v, 1, 1))
    sums[0] = sum_u
    sums[1] = sum_v
    if deep:
        sums[2] = deep_u
        sums[3] = deep_v


def layer_close(o_u, o_v, sums, mean, masks, depth, deep):
    if deep:
        depth[0] = 1.0 / sums[2]
        depth[1] = 1.0 / sums[3]
    for k, out in enumerate((o_u, o_v)):
        fix = (mean[k] * (1.0 / NSUB) - sums[k]) * depth[k]
        mask = masks[k]
        for l in range(out.shape[0]):
            out[l] = mask * (out[l] + fix)


def layer_edges(h_ref, v_ref, own_r, own_l, recv_w, recv_e, packs, o_h, o_u, o_v, mean, masks, depth, top, deep):
    layers, nx, ny = h_ref.shape
    up = own_l.shape[0]
    layer = iota((up, ny), 0)
    h_last, u_last, h_first = own_r[0:up], own_r[up:], own_l[...]
    h_e, h_w, u_w = recv_e[...], recv_w[0:up], recv_w[up:]
    hu = (h_last + h_e) * 0.5
    press = h_e - h_last
    step = 1
    while step < layers:
        press = press + jnp.where(layer >= step, roll(press, step, 0), 0.0)
        step *= 2
    trial = u_last - PRESS_COEF * press
    outflow = FLUX_STEP * (u_last * hu)
    inflow = FLUX_STEP * (u_w * ((h_w + h_first) * 0.5))
    whole = lambda a: jnp.sum(jnp.where(layer < layers, a, 0.0), axis=0, keepdims=True)
    if deep:
        depth[0, nx - 1 : nx, :] = 1.0 / whole(hu)
    fix = (mean[0, nx - 1 : nx, :] * (1.0 / NSUB) - whole(hu * trial)) * depth[0, nx - 1 : nx, :]
    edge_u = masks[0][nx - 1 : nx, :] * (trial + fix)
    for l in range(layers):
        o_u[l, nx - 1 : nx, :] = edge_u[l : l + 1]
        o_h[l, nx - 1 : nx, :] = o_h[l, nx - 1 : nx, :] - outflow[l : l + 1]
        o_h[l, 0:1, :] = o_h[l, 0:1, :] + inflow[l : l + 1]

    lane = iota((nx, LANES), 1)
    last = ny - LANES
    at_end = lane == LANES - 1
    at_start = jnp.logical_and(top, lane == 0)
    side = packs[0]
    cap = jnp.where(top, packs[1], side)
    press, total, deep_v = 0.0, 0.0, 0.0
    trials = []
    for l in range(layers):
        h, v = h_ref[l, :, last:ny], v_ref[l, :, last:ny]
        h_north = roll(cap, LANES - 1 - l, 1)
        hv = (h + h_north) * 0.5
        press = press + (h_north - h)
        trials.append(v - PRESS_COEF * press)
        total = total + hv * trials[l]
        deep_v = deep_v + hv
        o_h[l, :, last:ny] = o_h[l, :, last:ny] - jnp.where(at_end, FLUX_STEP * (v * hv), 0.0)
        h_south, v_south = roll(side, -l, 1), roll(side, -(layers + l), 1)
        inflow = FLUX_STEP * (v_south * ((h_south + h_ref[l, :, 0:LANES]) * 0.5))
        o_h[l, :, 0:LANES] = o_h[l, :, 0:LANES] + jnp.where(at_start, inflow, 0.0)
    if deep:
        depth[1, :, last:ny] = jnp.where(at_end, 1.0 / deep_v, depth[1, :, last:ny])
    fix = (mean[1, :, last:ny] * (1.0 / NSUB) - total) * depth[1, :, last:ny]
    for l in range(layers):
        edge_v = masks[1][:, last:ny] * (trials[l] + fix)
        o_v[l, :, last:ny] = jnp.where(at_end, edge_v, o_v[l, :, last:ny])


def last_kernel(flat, n_h, n_u, n_v, o_eta, o_bu, o_bv, o_h, o_u, o_v, sems):
    moves = [(flat.at[k], o, 0) for k, o in enumerate((o_eta, o_bu, o_bv))]
    moves += [(n_h, o_h, 1), (n_u, o_u, 2), (n_v, o_v, 3)]
    copies = [pltpu.make_async_copy(src, dst, sems.at[k]) for src, dst, k in moves]
    for copy in copies:
        copy.start()
    drain(flat, sems.at[0])
    for copy in copies[3:]:
        copy.wait()


def kernel(
    zonal_devices,
    merid_devices,
    height_any,
    trans_u_any,
    trans_v_any,
    thick_any,
    vel_u_any,
    vel_v_any,
    faces_any,
    seeds_any,
    scale_any,
    base_any,
    flat,
    o_h,
    o_u,
    o_v,
    thick,
    vel,
    faces,
    seeds,
    scale,
    mid_h,
    mid_u,
    mid_v,
    mean,
    sums,
    depth,
    X,
    G,
    D,
    F,
    wind_own,
    wind_far,
    west_send,
    west_recv,
    east_send,
    east_recv,
    spare_send,
    spare_recv,
    pack_send,
    inner_recv,
    fold_recv,
    lay_send_r,
    lay_send_l,
    lay_recv_w,
    lay_recv_e,
    lay_pack_send,
    lay_pack_recv,
    blank,
    load_sem,
    send_sem,
    recv_sem,
    lay_recv_sem,
    late_sem,
):
    layers, nx, ny = thick.shape
    Z = zonal_devices
    total_x, total_y = nx * Z, ny * merid_devices
    z = lax.axis_index("zonal")
    m = lax.axis_index("merid")
    other = 1 - m
    bottom = m == 0
    top = m == merid_devices - 1
    right, left = lax.rem(z + 1, Z), lax.rem(z + Z - 1, Z)
    mirror = Z - 1 - z
    mirror_e, mirror_w = lax.rem(mirror + 1, Z), lax.rem(mirror + Z - 1, Z)
    rows = nx + 2 * PAD
    width = ny + LANES
    last = ny - LANES
    own = slice(PAD, PAD + nx)
    lane = iota((nx, LANES), 1)

    barrier = pltpu.get_barrier_semaphore()
    first_z, last_z = z == 0, z == Z - 1
    late_left = jnp.logical_or(first_z, last_z)
    mirrors = (mirror_w, mirror, mirror_e)

    def greet(sem, zz, mm):
        pl.semaphore_signal(sem, inc=1, device_id={"zonal": zz, "merid": mm}, device_id_type=MESH)

    greet(barrier, z, other)
    for mm in (m, other):
        greet(barrier, left, mm)
        pl.when(z < Z - 2)(lambda mm=mm: greet(barrier, right, mm))

    for zz in mirrors:

        @pl.when(jnp.logical_and(top, zz > z))
        def _():
            greet(barrier, zz, m)

    moves = (
        (faces_any, faces),
        (height_any, X.at[0, own, 0:ny]),
        (trans_u_any, X.at[1, own, 0:ny]),
        (trans_v_any, X.at[2, own, 0:ny]),
        (base_any, X.at[6:8, own, 0:ny]),
        (thick_any, thick),
        (vel_u_any, vel.at[0]),
        (vel_v_any, vel.at[1]),
        (seeds_any, seeds),
        (scale_any, scale),
    )
    group = (0, 0, 0, 0, 0, 1, 2, 2, 3, 4)
    vel_u, vel_v = vel.at[0], vel.at[1]
    loads = [pltpu.make_async_copy(src, dst, load_sem.at[k]) for k, (src, dst) in zip(group, moves)]
    for load in loads:
        load.start()

    near = 3 + jnp.where(jnp.logical_or(first_z, last_z), 0, 2)
    lower = sum((zz < z).astype(jnp.int32) for zz in mirrors)
    upper = sum((zz > z).astype(jnp.int32) for zz in mirrors)
    pl.semaphore_wait(barrier, near + jnp.where(top, lower, 0))

    @pl.when(z >= Z - 2)
    def _():
        for mm in (m, other):
            greet(late_sem.at[0], right, mm)

    for zz in mirrors:

        @pl.when(jnp.logical_and(top, zz < z))
        def _():
            greet(late_sem.at[1], zz, m)

    drain(blank.at[0 : sum(lines(dst) for _, dst in moves[:5])], load_sem.at[0])
    X[3, own, 0:ny] = faces[0].astype(jnp.float32)
    X[4, own, 0:ny] = faces[1].astype(jnp.float32)

    blocks = ny // LANES
    full_east = sum(EAST) // 8 * 8

    def pack_rows(step, start, stop):
        west = sum(WEST[f] for f in ORDER[:start])
        east = sum(EAST[f] for f in ORDER[:start])
        for f in ORDER[start:stop]:
            west_send[step, west : west + WEST[f], :] = X[f, PAD + nx - WEST[f] : PAD + nx, 0:ny]
            fits = EAST[f] if step else min(EAST[f], full_east - east)
            east_send[step, east : east + fits, :] = X[f, PAD : PAD + fits, 0:ny]
            for q in range(fits, EAST[f]):
                for t in range(blocks):
                    at = (q - fits) * blocks + t
                    spare_send[at : at + 1, :] = X[f, PAD + q : PAD + q + 1, t * LANES : (t + 1) * LANES]
            west += WEST[f]
            east += EAST[f]

    def pack_edges(step, fields, between=lambda: None):
        inner = jnp.zeros((nx, LANES), jnp.float32)
        crest = jnp.zeros((nx, LANES), jnp.float32)
        for f in range(fields):
            here = jnp.logical_and(lane >= f * SLOT, lane < (f + 1) * SLOT)
            high = roll(X[f, own, last:ny], SLOT * (f + 1), 1)
            low = roll(X[f, own, 0:LANES], SLOT * f, 1)
            crest = jnp.where(here, high, crest)
            inner = jnp.where(here, jnp.where(bottom, high, low), inner)
        pack_send[step, 0] = inner
        between()
        pack_send[step, 2] = crest
        for r in range(nx):
            pack_send[step, 1, r : r + 1, :] = pack_send[step, 2, nx - 1 - r : nx - r, :]

    leaving = {}

    def send_tile(step, fields):
        def send(src, dst, k, zz, mm):
            leaving[k] = leaving.get(k, 0) + lines(src)
            return pltpu.make_async_remote_copy(
                src_ref=src,
                dst_ref=dst,
                send_sem=send_sem.at[k],
                recv_sem=recv_sem.at[step],
                device_id={"zonal": zz, "merid": mm},
                device_id_type=MESH,
            )

        def rows_of(src, dst, k, zz, count):
            cuts = [0, CUT, count] if count > CUT else [0, count]
            parts = [slice(low, high) for low, high in zip(cuts[:-1], cuts[1:])]
            return [send(src.at[step, p], dst.at[step, p], k, zz, m) for p in parts]

        tail, whole, start = slice(nx - PAD, nx), slice(0, nx), slice(0, PAD)
        places = (slice(0, PAD), own, slice(PAD + nx, rows))
        inner = lambda s, part: (pack_send.at[step, 0, part], inner_recv.at[step, places[s]])
        west = rows_of(west_send, west_recv, 0, right, tile_up(sum(WEST[:fields])))
        east = rows_of(east_send, east_recv, int(step == 0), left, tile_up(sum(EAST[:fields])) if step else full_east)
        if not step:
            east.append(send(spare_send, spare_recv, 1, left, m))
        west.append(send(*inner(0, tail), 0, right, other))
        east.append(send(*inner(2, start), int(step == 0), left, other))
        across = send(*inner(1, whole), 0, z, other)
        folds = []
        for s, part, zz in ((2, start, mirror_w), (1, whole, mirror), (0, tail, mirror_e)):
            src, dst = pack_send.at[step, 1, part], fold_recv.at[step, places[s]]
            near = pltpu.make_async_copy(src, dst, recv_sem.at[step])
            folds.append((send(src, dst, 2 + s, zz, m), near, zz))
        return west, east, across, folds

    even = lax.rem(z, 2) == 0

    def start_all(copies):
        for copy in copies:
            copy.start()

    far_west, far_east = jnp.logical_not(even), jnp.logical_and(even, jnp.logical_not(first_z))

    def each(west_when, east_when, act, tile):
        pl.when(west_when)(lambda: act(tile[0]))
        pl.when(east_when)(lambda: act(tile[1]))

    def start_folds(folds, chosen):
        for far_copy, _, zz in folds:
            pl.when(jnp.logical_and(top, chosen(zz)))(far_copy.start)

    def take(sem, always, at_top):
        pl.when(bottom)(lambda: drain(blank.at[0:always], sem))
        pl.when(top)(lambda: drain(blank.at[0 : always + at_top], sem))

    def take_tile(step, fields):
        count = tile_up(sum(WEST[:fields])) + (tile_up(sum(EAST[:fields])) if step else full_east)
        take(recv_sem.at[step], count * blocks + rows + (0 if step else lines(spare_recv)), rows)

        west = east = 0
        for f in ORDER[:fields]:
            X[f, PAD - WEST[f] : PAD, 0:ny] = west_recv[step, west : west + WEST[f], :]
            fits = EAST[f] if step else min(EAST[f], full_east - east)
            X[f, PAD + nx : PAD + nx + fits, 0:ny] = east_recv[step, east : east + fits, :]
            for q in range(fits, EAST[f]):
                for t in range(blocks):
                    at, row = (q - fits) * blocks + t, PAD + nx + q
                    X[f, row : row + 1, t * LANES : (t + 1) * LANES] = spare_recv[at : at + 1, :]
            west += WEST[f]
            east += EAST[f]
        for f in range(fields):
            got = inner_recv[step]
            X[f, :, ny:width] = jnp.where(
                top, roll(got, LANES - SLOT * (f + 1), 1), roll(got, LANES - SLOT * f, 1)
            )
            G[f] = roll(fold_recv[step], LANES - SLOT * (f + 1), 1)

    pack_rows(0, 0, FIELDS - 1)
    tile = tile_0 = send_tile(0, FIELDS)
    lead = (jnp.logical_or(far_west, first_z), far_east)
    each(*lead, lambda c: c[0].start(), tile)
    loads[5].wait()
    total = thick[0]
    for l in range(1, layers):
        total = total + thick[l]
    X[5, own, 0:ny] = (WAVE_LIMIT / layers) * total
    pack_rows(0, FIELDS - 1, FIELDS)
    pack_edges(0, FIELDS)
    each(*lead, lambda c: start_all(c[1:]), tile)
    each(far_east, jnp.logical_and(far_west, jnp.logical_not(last_z)), start_all, tile)
    tile[2].start()
    start_folds(tile[3], lambda zz: zz < z)
    for _, near_copy, zz in tile[3]:
        pl.when(jnp.logical_and(top, zz == z))(near_copy.start)

    def lay_copies(step):
        def one(src, dst, zz, mm, k=0):
            leaving[k] = leaving.get(k, 0) + lines(src)
            return pltpu.make_async_remote_copy(
                src_ref=src,
                dst_ref=dst,
                send_sem=send_sem.at[k],
                recv_sem=lay_recv_sem.at[step],
                device_id={"zonal": zz, "merid": mm},
                device_id_type=MESH,
            )

        return [
            one(lay_send_r.at[step], lay_recv_w.at[step], right, m),
            one(lay_send_l.at[step], lay_recv_e.at[step], left, m),
            one(lay_pack_send.at[step, 0], lay_pack_recv.at[step, 0], z, other),
            one(lay_pack_send.at[step, 1], lay_pack_recv.at[step, 1], mirror, m, 3),
        ]

    above = lay_send_r.shape[1] // 2

    def send_layers(step, h_ref, u_ref, v_ref):
        edge = jnp.zeros((nx, LANES), jnp.float32)
        brim = jnp.zeros((nx, LANES), jnp.float32)
        for l in range(layers):
            lay_send_r[step, l : l + 1, :] = h_ref[l, nx - 1 : nx, :]
            lay_send_r[step, above + l : above + l + 1, :] = u_ref[l, nx - 1 : nx, :]
            lay_send_l[step, l : l + 1, :] = h_ref[l, 0:1, :]
            high = roll(h_ref[l, :, last:ny], l + 1, 1)
            low = roll(h_ref[l, :, 0:LANES], l, 1)
            high_v = roll(v_ref[l, :, last:ny], layers + l + 1, 1)
            edge = jnp.where(lane == l, jnp.where(bottom, high, low), edge)
            edge = jnp.where(lane == layers + l, high_v, edge)
            brim = jnp.where(lane == l, high, brim)
        lay_pack_send[step, 0] = edge
        lay_pack_send[step, 2] = brim
        for r in range(nx):
            lay_pack_send[step, 1, r : r + 1, :] = lay_pack_send[step, 2, nx - 1 - r : nx - r, :]
        return lay_copies(step)

    def start_layers(out, first):
        out[2].start()
        hold, late_fold = (late_left, mirror > z) if first else (False, False)
        pl.when(jnp.logical_and(top, jnp.logical_not(late_fold)))(out[3].start)
        pl.when(far_west)(out[0].start)
        pl.when(jnp.logical_not(hold))(out[1].start)
        pl.when(jnp.logical_not(far_west))(out[0].start)

    def wait_layers(step):
        take(lay_recv_sem.at[step], lines(lay_recv_w.at[step]) + lines(lay_recv_e.at[step]) + nx, nx)

    def wait_sent():
        drain(blank.at[0 : leaving[0]], send_sem.at[0])
        pl.when(jnp.logical_not(first_z))(lambda: drain(blank.at[0 : leaving[1]], send_sem.at[1]))
        for k, zz in zip((4, 3, 2), mirrors):
            pl.when(jnp.logical_and(top, zz != z))(lambda k=k: drain(blank.at[0 : leaving[k]], send_sem.at[k]))

    drain(vel, load_sem.at[2])
    for load in loads[8:]:
        load.wait()
    out = send_layers(0, thick, vel_u, vel_v)

    start_layers(out, True)
    first = (z * nx - PAD).astype(jnp.float32)
    col = first + iota((rows, 1), 0).astype(jnp.float32) + float(total_x)
    far_col = float(2 * total_x - 1) - (first + iota((rows, 1), 0).astype(jnp.float32))
    spot = iota((1, width), 1)
    row = spot + m * ny
    row = jnp.where(jnp.logical_and(top, spot >= ny), row - width, row).astype(jnp.float32)
    far_row = (iota((1, LANES), 1) + (total_y - LANES)).astype(jnp.float32)
    px = jnp.zeros((rows, width), jnp.float32)
    py = jnp.zeros((rows, width), jnp.float32)
    fx = jnp.zeros((rows, LANES), jnp.float32)
    fy = jnp.zeros((rows, LANES), jnp.float32)
    for k in range(seeds.shape[1]):
        seed_x = seeds[0, k].astype(jnp.float32)
        seed_y = seeds[1, k].astype(jnp.float32)
        ca, sa = turns(seed_x, col, total_x)
        cf, sf = turns(seed_x, far_col, total_x)
        cb, sb = turns(seed_y, row, total_y)
        cg, sg = turns(seed_y, far_row, total_y)
        amp = scale[k]
        ca, sa, cf, sf = amp * ca, amp * sa, amp * cf, amp * sf
        px = px + (ca * cb - sa * sb)
        py = py + (sa * cb + ca * sb)
        fx = fx + (cf * cg - sf * sg)
        fy = fy + (sf * cg + cf * sg)
    wind_own[0] = px
    wind_own[1] = py
    wind_far[0] = fx
    wind_far[1] = fy

    layer_trial(thick, vel_u, vel_v, mid_h, mid_u, mid_v, sums, True)

    @pl.when(late_left)
    def _():
        pl.semaphore_wait(late_sem.at[0], 2)
        start_all(tile[1])


    @pl.when(jnp.logical_and(top, upper > 0))
    def _():
        pl.semaphore_wait(late_sem.at[1], upper)

    start_folds(tile[3], lambda zz: zz > z)
    pl.when(jnp.logical_and(top, mirror > z))(out[3].start)

    @pl.when(first_z)
    def _():
        drain(blank.at[0 : leaving[1]], send_sem.at[1])

    pl.when(late_left)(out[1].start)

    take_tile(0, FIELDS)
    lanes = iota((rows, width), 1)
    wall = jnp.logical_and(bottom, lanes == 0)
    crown = jnp.logical_and(top, iota((rows, LANES), 1) == LANES - 1)
    far_top = iota((rows, LANES), 1) == LANES - 1

    def southern(bv, g_bv):
        return jnp.where(wall, 0.0, roll(bv, 1, 1)), roll(g_bv, 1, 1)

    for k in range(2):
        mask, far_mask = X[3 + k], G[3 + k]
        D[2 * k] = mask * X[5]
        F[2 * k] = far_mask * G[5]
        D[2 * k + 1] = mask * (STRESS_SCALE * (X[6 + k] + wind_own[k]))
        F[2 * k + 1] = far_mask * (STRESS_SCALE * (G[6 + k] + wind_far[k]))
    for k in range(2):
        D[4 + k], F[4 + k] = southern(D[2 + k], F[2 + k])

    def close_step(step, h_ref, v_ref, n_h, n_u, n_v):
        layer_edges(
            h_ref, v_ref, lay_send_r.at[step], lay_send_l.at[step], lay_recv_w.at[step], lay_recv_e.at[step],
            lay_pack_recv.at[step], n_h, n_u, n_v, mean, masks, depth, top, step == 0,
        )

    def substep(carry, masked):
        eta, bu, bv, south_v, g_eta, g_bu, g_bv, g_south_v = carry
        eta = eta - (bu - roll(bu, 1, 0) + bv - south_v)
        g_eta = g_eta - (g_bu - roll(g_bu, -1, 0) + g_bv - g_south_v)
        if masked:
            bu, bv, south_v, g_bu, g_bv, g_south_v = masked
        north, south = roll(eta, -1, 1), roll(eta, 1, 1)
        brink = jnp.where(crown, g_eta[:, LANES - 1 :], north[:, last:ny])
        north = jnp.concatenate([north[:, :last], brink, north[:, ny:]], axis=1)
        g_north = jnp.where(far_top, eta[:, ny - 1 : ny], roll(g_eta, -1, 1))
        g_south = roll(g_eta, 1, 1)
        bu = bu - D[0] * (roll(eta, -1, 0) - eta) + D[1]
        bv = bv - D[2] * (north - eta) + D[3]
        south_v = south_v - D[4] * (eta - south) + D[5]
        g_bu = g_bu - F[0] * (roll(g_eta, 1, 0) - g_eta) + F[1]
        g_bv = g_bv - F[2] * (g_north - g_eta) + F[3]
        g_south_v = g_south_v - F[4] * (g_eta - g_south) + F[5]
        mean[0] = mean[0] + bu[own, 0:ny]
        mean[1] = mean[1] + bv[own, 0:ny]
        return eta, bu, bv, south_v, g_eta, g_bu, g_bv, g_south_v

    def substeps(out, raw):
        mean[...] = jnp.zeros((2, nx, ny), jnp.float32)
        bu, bv, g_bu, g_bv = X[1], X[2], G[1], G[2]
        south_v, g_south_v = southern(bv, g_bv)
        carry = X[0], bu, bv, south_v, G[0], g_bu, g_bv, g_south_v
        masked = None
        if raw:
            bu, bv, g_bu, g_bv = X[3] * bu, X[4] * bv, G[3] * g_bu, G[4] * g_bv
            south_v, g_south_v = southern(bv, g_bv)
            masked = bu, bv, south_v, g_bu, g_bv, g_south_v
        for n in range(NSUB):
            carry = substep(carry, masked if n == 0 else None)
        for k in range(3):
            out[k, ...] = carry[k][own, 0:ny]

    masks = X[3, own, 0:ny], X[4, own, 0:ny]
    h_ref, u_ref, v_ref = thick, vel_u, vel_v
    n_h, n_u, n_v = mid_h, mid_u, mid_v
    for step in range(STEPS - 1):
        substeps(X.at[0:3, own, 0:ny], step == 0)
        pack_rows(step + 1, 0, 3)
        tile = send_tile(step + 1, 3)
        lead = (far_west, even)
        each(*lead, lambda c: start_all(c[:-1]), tile)

        def inner_ready():
            each(*lead, lambda c: c[-1].start(), tile)
            tile[2].start()

        pack_edges(step + 1, 3, inner_ready)
        start_folds(tile[3], lambda zz: zz != z)
        for _, near_copy, zz in tile[3]:
            pl.when(jnp.logical_and(top, zz == z))(near_copy.start)
        each(even, far_west, start_all, tile)
        layer_close(n_u, n_v, sums, mean, masks, depth, step == 0)
        wait_layers(step)
        close_step(step, h_ref, v_ref, n_h, n_u, n_v)
        h_ref, u_ref, v_ref = n_h, n_u, n_v
        n_h, n_u, n_v = o_h, o_u, o_v
        out = send_layers(step + 1, h_ref, u_ref, v_ref)
        start_layers(out, False)
        layer_trial(h_ref, u_ref, v_ref, n_h, n_u, n_v, sums, False)
        take_tile(step + 1, 3)
    substeps(flat, STEPS == 1)
    layer_close(n_u, n_v, sums, mean, masks, depth, False)
    wait_layers(STEPS - 1)
    close_step(STEPS - 1, h_ref, v_ref, n_h, n_u, n_v)
    wait_sent()


def body(zonal_devices, merid_devices, *args):
    thickness = args[3]
    layers, nx, ny = thickness.shape
    up = tile_up(layers)
    f32 = jnp.float32
    vmem = pl.BlockSpec(memory_space=pltpu.VMEM)
    far = pl.BlockSpec(memory_space=pltpu.HBM)
    hbm = pl.BlockSpec(memory_space=pl.ANY)
    rows = nx + 2 * PAD
    west, east = tile_up(sum(WEST)), tile_up(sum(EAST))
    spare = tile_up(sum(EAST) % 8 * ny // LANES)
    plane = jax.ShapeDtypeStruct((nx, ny), f32)
    solid = jax.ShapeDtypeStruct((layers, nx, ny), f32)
    kept = [(3, nx, ny), (layers, nx, ny), (layers, nx, ny), (layers, nx, ny)]
    room = sum(math.prod(shape) for shape in kept)
    args = list(args)
    args[7] = args[7].T
    between = pl.pallas_call(
        functools.partial(kernel, zonal_devices, merid_devices),
        out_shape=[pltpu.VMEM(shape, f32) for shape in kept],
        in_specs=[far] * 10,
        out_specs=[vmem] * len(kept),
        scratch_shapes=[
            pltpu.VMEM((layers, nx, ny), f32),
            pltpu.VMEM((2, layers, nx, ny), f32),
            pltpu.VMEM((2, nx, ny), jnp.int32),
            pltpu.SMEM(args[7].shape, jnp.int32),
            pltpu.SMEM(args[8].shape, f32),
            pltpu.VMEM((layers, nx, ny), f32),
            pltpu.VMEM((layers, nx, ny), f32),
            pltpu.VMEM((layers, nx, ny), f32),
            pltpu.VMEM((2, nx, ny), f32),
            pltpu.VMEM((4, nx, ny), f32),
            pltpu.VMEM((2, nx, ny), f32),
            pltpu.VMEM((FIELDS, rows, ny + LANES), f32),
            pltpu.VMEM((FIELDS, rows, LANES), f32),
            pltpu.VMEM((6, rows, ny + LANES), f32),
            pltpu.VMEM((6, rows, LANES), f32),
            pltpu.VMEM((2, rows, ny + LANES), f32),
            pltpu.VMEM((2, rows, LANES), f32),
            pltpu.VMEM((STEPS, west, ny), f32),
            pltpu.VMEM((STEPS, west, ny), f32),
            pltpu.VMEM((STEPS, east, ny), f32),
            pltpu.VMEM((STEPS, east, ny), f32),
            pltpu.VMEM((spare, LANES), f32),
            pltpu.VMEM((spare, LANES), f32),
            pltpu.VMEM((STEPS, 3, nx, LANES), f32),
            pltpu.VMEM((STEPS, rows, LANES), f32),
            pltpu.VMEM((STEPS, rows, LANES), f32),
            pltpu.VMEM((STEPS, 2 * up, ny), f32),
            pltpu.VMEM((STEPS, up, ny), f32),
            pltpu.VMEM((STEPS, 2 * up, ny), f32),
            pltpu.VMEM((STEPS, up, ny), f32),
            pltpu.VMEM((STEPS, 3, nx, LANES), f32),
            pltpu.VMEM((STEPS, 2, nx, LANES), f32),
            pltpu.VMEM((4 * (west + east) * ny // LANES, LANES), f32),
            pltpu.SemaphoreType.DMA((5,)),
            pltpu.SemaphoreType.DMA((5,)),
            pltpu.SemaphoreType.DMA((STEPS,)),
            pltpu.SemaphoreType.DMA((STEPS,)),
            pltpu.SemaphoreType.REGULAR((2,)),
        ],
        compiler_params=pltpu.CompilerParams(
            collective_id=0, has_side_effects=True, vmem_limit_bytes=VMEM_BYTES - 4 * room - SPARE
        ),
        name="ocean",
    )(*args)
    return pl.pallas_call(
        last_kernel,
        out_shape=(plane, plane, plane, solid, solid, solid),
        in_specs=[vmem] * len(kept),
        out_specs=[hbm] * 6,
        scratch_shapes=[pltpu.SemaphoreType.DMA((4,))],
        compiler_params=pltpu.CompilerParams(vmem_limit_bytes=24 * 1024 * 1024),
        name="last",
    )(*between)


def solution(mesh):
    field = P(("members", "zonal"), "merid")
    solid = P(None, ("members", "zonal"), "merid")
    fixed = P(None, "zonal", "merid")
    return jax.shard_map(
        functools.partial(body, mesh.shape["zonal"], mesh.shape["merid"]),
        mesh=mesh,
        in_specs=(
            field, field, field, solid, solid, solid, fixed, P("members", None), P("members"), fixed,
        ),
        out_specs=(field, field, field, solid, solid, solid),
        check_vma=False,
    )
```

```python
import functools
import math

import jax
import jax.numpy as jnp
from jax import lax
from jax.experimental import pallas as pl
from jax.experimental.pallas import tpu as pltpu
from jax.sharding import PartitionSpec as P

NSUB = 6
STEPS = 2
MARGIN = NSUB
PAD = 8

WAVE_LIMIT = 0.225
STRESS_SCALE = 0.1
FLUX_STEP = 0.05
PRESS_COEF = 0.05
LANES = 128
VMEM_BYTES = 67043328
SPARE = 1 << 15
FIELDS = 8
SLOT = LANES // FIELDS
WEST = (NSUB - 1, NSUB, NSUB - 1, NSUB - 1, NSUB - 2, NSUB - 1, NSUB - 1, NSUB - 2)
EAST = (NSUB, NSUB, NSUB) + (NSUB - 1,) * 5
ORDER = (0, 1, 2, 3, 4, 6, 7, 5)
CUT = 32
MESH = pl.DeviceIdType.MESH


def roll(value, shift, axis):
    return pltpu.roll(value, shift % value.shape[axis], axis)


def iota(shape, axis):
    return lax.broadcasted_iota(jnp.int32, shape, axis)


def turns(seed, index, total):
    part = seed * index * (1.0 / total)
    angle = (2.0 * math.pi) * (part - jnp.floor(part))
    return jnp.cos(angle), jnp.sin(angle)


def lines(ref):
    return math.prod(ref.shape) // LANES


def drain(ref, sem):
    pltpu.make_async_copy(ref, ref, sem).wait()


def tile_up(count):
    return -(-count // 8) * 8


def layer_trial(h_ref, u_ref, v_ref, o_h, o_u, o_v, sums, deep):
    layers, nx, ny = h_ref.shape
    at_east = iota((nx, ny), 0) == nx - 1
    at_north = iota((nx, ny), 1) == ny - 1
    zero = jnp.zeros((nx, ny), jnp.float32)
    press_u, press_v, sum_u, sum_v = zero, zero, zero, zero
    deep_u, deep_v = zero, zero
    for l in range(layers):
        h, u, v = h_ref[l], u_ref[l], v_ref[l]
        h_east, h_north = roll(h, -1, 0), roll(h, -1, 1)
        hu = (h + h_east) * 0.5
        hv = (h + h_north) * 0.5
        if deep:
            deep_u = deep_u + hu
            deep_v = deep_v + hv
        flux_u = jnp.where(at_east, 0.0, u * hu)
        flux_v = jnp.where(at_north, 0.0, v * hv)
        press_u = press_u + (h_east - h)
        press_v = press_v + (h_north - h)
        trial_u = u - PRESS_COEF * press_u
        trial_v = v - PRESS_COEF * press_v
        sum_u = sum_u + hu * trial_u
        sum_v = sum_v + hv * trial_v
        o_u[l] = trial_u
        o_v[l] = trial_v
        o_h[l] = h - FLUX_STEP * (flux_u - roll(flux_u, 1, 0) + flux_v - roll(flux_v, 1, 1))
    sums[0] = sum_u
    sums[1] = sum_v
    if deep:
        sums[2] = deep_u
        sums[3] = deep_v


def layer_close(o_u, o_v, sums, mean, masks, depth, deep):
    if deep:
        depth[0] = 1.0 / sums[2]
        depth[1] = 1.0 / sums[3]
    for k, out in enumerate((o_u, o_v)):
        fix = (mean[k] * (1.0 / NSUB) - sums[k]) * depth[k]
        mask = masks[k]
        for l in range(out.shape[0]):
            out[l] = mask * (out[l] + fix)


def layer_edges(h_ref, v_ref, own_r, own_l, recv_w, recv_e, packs, o_h, o_u, o_v, mean, masks, depth, top, deep):
    layers, nx, ny = h_ref.shape
    up = own_l.shape[0]
    layer = iota((up, ny), 0)
    h_last, u_last, h_first = own_r[0:up], own_r[up:], own_l[...]
    h_e, h_w, u_w = recv_e[...], recv_w[0:up], recv_w[up:]
    hu = (h_last + h_e) * 0.5
    press = h_e - h_last
    step = 1
    while step < layers:
        press = press + jnp.where(layer >= step, roll(press, step, 0), 0.0)
        step *= 2
    trial = u_last - PRESS_COEF * press
    outflow = FLUX_STEP * (u_last * hu)
    inflow = FLUX_STEP * (u_w * ((h_w + h_first) * 0.5))
    whole = lambda a: jnp.sum(jnp.where(layer < layers, a, 0.0), axis=0, keepdims=True)
    if deep:
        depth[0, nx - 1 : nx, :] = 1.0 / whole(hu)
    fix = (mean[0, nx - 1 : nx, :] * (1.0 / NSUB) - whole(hu * trial)) * depth[0, nx - 1 : nx, :]
    edge_u = masks[0][nx - 1 : nx, :] * (trial + fix)
    for l in range(layers):
        o_u[l, nx - 1 : nx, :] = edge_u[l : l + 1]
        o_h[l, nx - 1 : nx, :] = o_h[l, nx - 1 : nx, :] - outflow[l : l + 1]
        o_h[l, 0:1, :] = o_h[l, 0:1, :] + inflow[l : l + 1]

    lane = iota((nx, LANES), 1)
    last = ny - LANES
    at_end = lane == LANES - 1
    at_start = jnp.logical_and(top, lane == 0)
    side = packs[0]
    cap = jnp.where(top, packs[1], side)
    press, total, deep_v = 0.0, 0.0, 0.0
    trials = []
    for l in range(layers):
        h, v = h_ref[l, :, last:ny], v_ref[l, :, last:ny]
        h_north = roll(cap, LANES - 1 - l, 1)
        hv = (h + h_north) * 0.5
        press = press + (h_north - h)
        trials.append(v - PRESS_COEF * press)
        total = total + hv * trials[l]
        deep_v = deep_v + hv
        o_h[l, :, last:ny] = o_h[l, :, last:ny] - jnp.where(at_end, FLUX_STEP * (v * hv), 0.0)
        h_south, v_south = roll(side, -l, 1), roll(side, -(layers + l), 1)
        inflow = FLUX_STEP * (v_south * ((h_south + h_ref[l, :, 0:LANES]) * 0.5))
        o_h[l, :, 0:LANES] = o_h[l, :, 0:LANES] + jnp.where(at_start, inflow, 0.0)
    if deep:
        depth[1, :, last:ny] = jnp.where(at_end, 1.0 / deep_v, depth[1, :, last:ny])
    fix = (mean[1, :, last:ny] * (1.0 / NSUB) - total) * depth[1, :, last:ny]
    for l in range(layers):
        edge_v = masks[1][:, last:ny] * (trials[l] + fix)
        o_v[l, :, last:ny] = jnp.where(at_end, edge_v, o_v[l, :, last:ny])


def last_kernel(flat, n_h, n_u, n_v, o_eta, o_bu, o_bv, o_h, o_u, o_v, sems):
    moves = [(flat.at[k], o, 0) for k, o in enumerate((o_eta, o_bu, o_bv))]
    moves += [(n_h, o_h, 1), (n_u, o_u, 2), (n_v, o_v, 3)]
    copies = [pltpu.make_async_copy(src, dst, sems.at[k]) for src, dst, k in moves]
    for copy in copies:
        copy.start()
    drain(flat, sems.at[0])
    for copy in copies[3:]:
        copy.wait()


def kernel(
    zonal_devices,
    merid_devices,
    height_any,
    trans_u_any,
    trans_v_any,
    thick_any,
    vel_u_any,
    vel_v_any,
    faces_any,
    seeds_any,
    scale_any,
    base_any,
    flat,
    o_h,
    o_u,
    o_v,
    thick,
    vel,
    faces,
    seeds,
    scale,
    mid_h,
    mid_u,
    mid_v,
    mean,
    sums,
    depth,
    X,
    G,
    D,
    F,
    wind_own,
    wind_far,
    west_send,
    west_recv,
    east_send,
    east_recv,
    spare_send,
    spare_recv,
    pack_send,
    inner_recv,
    fold_recv,
    lay_send_r,
    lay_send_l,
    lay_recv_w,
    lay_recv_e,
    lay_pack_send,
    lay_pack_recv,
    blank,
    load_sem,
    send_sem,
    recv_sem,
    lay_recv_sem,
    late_sem,
):
    layers, nx, ny = thick.shape
    Z = zonal_devices
    total_x, total_y = nx * Z, ny * merid_devices
    z = lax.axis_index("zonal")
    m = lax.axis_index("merid")
    other = 1 - m
    bottom = m == 0
    top = m == merid_devices - 1
    right, left = lax.rem(z + 1, Z), lax.rem(z + Z - 1, Z)
    mirror = Z - 1 - z
    mirror_e, mirror_w = lax.rem(mirror + 1, Z), lax.rem(mirror + Z - 1, Z)
    rows = nx + 2 * PAD
    width = ny + LANES
    last = ny - LANES
    own = slice(PAD, PAD + nx)
    lane = iota((nx, LANES), 1)

    barrier = pltpu.get_barrier_semaphore()
    first_z, last_z = z == 0, z == Z - 1
    late_left = jnp.logical_or(first_z, last_z)
    mirrors = (mirror_w, mirror, mirror_e)

    def greet(sem, zz, mm):
        pl.semaphore_signal(sem, inc=1, device_id={"zonal": zz, "merid": mm}, device_id_type=MESH)

    greet(barrier, z, other)
    for mm in (m, other):
        greet(barrier, left, mm)
        pl.when(z < Z - 2)(lambda mm=mm: greet(barrier, right, mm))

    for zz in mirrors:

        @pl.when(jnp.logical_and(top, zz > z))
        def _():
            greet(barrier, zz, m)

    moves = (
        (faces_any, faces),
        (height_any, X.at[0, own, 0:ny]),
        (trans_u_any, X.at[1, own, 0:ny]),
        (trans_v_any, X.at[2, own, 0:ny]),
        (base_any, X.at[6:8, own, 0:ny]),
        (thick_any, thick),
        (vel_u_any, vel.at[0]),
        (vel_v_any, vel.at[1]),
        (seeds_any, seeds),
        (scale_any, scale),
    )
    group = (0, 0, 0, 0, 0, 1, 2, 2, 3, 4)
    vel_u, vel_v = vel.at[0], vel.at[1]
    loads = [pltpu.make_async_copy(src, dst, load_sem.at[k]) for k, (src, dst) in zip(group, moves)]
    for load in loads:
        load.start()

    near = 3 + jnp.where(jnp.logical_or(first_z, last_z), 0, 2)
    lower = sum((zz < z).astype(jnp.int32) for zz in mirrors)
    upper = sum((zz > z).astype(jnp.int32) for zz in mirrors)
    pl.semaphore_wait(barrier, near + jnp.where(top, lower, 0))

    @pl.when(z >= Z - 2)
    def _():
        for mm in (m, other):
            greet(late_sem.at[0], right, mm)

    for zz in mirrors:

        @pl.when(jnp.logical_and(top, zz < z))
        def _():
            greet(late_sem.at[1], zz, m)

    drain(blank.at[0 : sum(lines(dst) for _, dst in moves[:5])], load_sem.at[0])
    X[3, own, 0:ny] = faces[0].astype(jnp.float32)
    X[4, own, 0:ny] = faces[1].astype(jnp.float32)

    blocks = ny // LANES
    full_east = sum(EAST) // 8 * 8

    def pack_rows(step, start, stop):
        west = sum(WEST[f] for f in ORDER[:start])
        east = sum(EAST[f] for f in ORDER[:start])
        for f in ORDER[start:stop]:
            west_send[step, west : west + WEST[f], :] = X[f, PAD + nx - WEST[f] : PAD + nx, 0:ny]
            fits = EAST[f] if step else min(EAST[f], full_east - east)
            east_send[step, east : east + fits, :] = X[f, PAD : PAD + fits, 0:ny]
            for q in range(fits, EAST[f]):
                for t in range(blocks):
                    at = (q - fits) * blocks + t
                    spare_send[at : at + 1, :] = X[f, PAD + q : PAD + q + 1, t * LANES : (t + 1) * LANES]
            west += WEST[f]
            east += EAST[f]

    def pack_edges(step, fields, between=lambda: None):
        inner = jnp.zeros((nx, LANES), jnp.float32)
        crest = jnp.zeros((nx, LANES), jnp.float32)
        for f in range(fields):
            here = jnp.logical_and(lane >= f * SLOT, lane < (f + 1) * SLOT)
            high = roll(X[f, own, last:ny], SLOT * (f + 1), 1)
            low = roll(X[f, own, 0:LANES], SLOT * f, 1)
            crest = jnp.where(here, high, crest)
            inner = jnp.where(here, jnp.where(bottom, high, low), inner)
        pack_send[step, 0] = inner
        between()
        pack_send[step, 2] = crest
        for r in range(nx):
            pack_send[step, 1, r : r + 1, :] = pack_send[step, 2, nx - 1 - r : nx - r, :]

    leaving = {}

    def send_tile(step, fields):
        def send(src, dst, k, zz, mm):
            leaving[k] = leaving.get(k, 0) + lines(src)
            return pltpu.make_async_remote_copy(
                src_ref=src,
                dst_ref=dst,
                send_sem=send_sem.at[k],
                recv_sem=recv_sem.at[step],
                device_id={"zonal": zz, "merid": mm},
                device_id_type=MESH,
            )

        def rows_of(src, dst, k, zz, count):
            cuts = [0, CUT, count] if count > CUT else [0, count]
            parts = [slice(low, high) for low, high in zip(cuts[:-1], cuts[1:])]
            return [send(src.at[step, p], dst.at[step, p], 5 * k if n else k, zz, m) for n, p in enumerate(parts)]

        tail, whole, start = slice(nx - PAD, nx), slice(0, nx), slice(0, PAD)
        places = (slice(0, PAD), own, slice(PAD + nx, rows))
        inner = lambda s, part: (pack_send.at[step, 0, part], inner_recv.at[step, places[s]])
        west = rows_of(west_send, west_recv, 0, right, tile_up(sum(WEST[:fields])))
        east = rows_of(east_send, east_recv, int(step == 0), left, tile_up(sum(EAST[:fields])) if step else full_east)
        if not step:
            east.append(send(spare_send, spare_recv, 5, left, m))
        west.append(send(*inner(0, tail), 0, right, other))
        east.append(send(*inner(2, start), 0 if step else 5, left, other))
        across = send(*inner(1, whole), 0, z, other)
        folds = []
        for s, part, zz in ((2, start, mirror_w), (1, whole, mirror), (0, tail, mirror_e)):
            src, dst = pack_send.at[step, 1, part], fold_recv.at[step, places[s]]
            near = pltpu.make_async_copy(src, dst, recv_sem.at[step])
            folds.append((send(src, dst, 2 + s, zz, m), near, zz))
        return west, east, across, folds

    even = lax.rem(z, 2) == 0

    def start_all(copies):
        for copy in copies:
            copy.start()

    far_west, far_east = jnp.logical_not(even), jnp.logical_and(even, jnp.logical_not(first_z))

    def each(west_when, east_when, act, tile):
        pl.when(west_when)(lambda: act(tile[0]))
        pl.when(east_when)(lambda: act(tile[1]))

    def start_folds(folds, chosen):
        for far_copy, _, zz in folds:
            pl.when(jnp.logical_and(top, chosen(zz)))(far_copy.start)

    def take(sem, always, at_top):
        pl.when(bottom)(lambda: drain(blank.at[0:always], sem))
        pl.when(top)(lambda: drain(blank.at[0 : always + at_top], sem))

    def take_tile(step, fields):
        count = tile_up(sum(WEST[:fields])) + (tile_up(sum(EAST[:fields])) if step else full_east)
        take(recv_sem.at[step], count * blocks + rows + (0 if step else lines(spare_recv)), rows)

        west = east = 0
        for f in ORDER[:fields]:
            X[f, PAD - WEST[f] : PAD, 0:ny] = west_recv[step, west : west + WEST[f], :]
            fits = EAST[f] if step else min(EAST[f], full_east - east)
            X[f, PAD + nx : PAD + nx + fits, 0:ny] = east_recv[step, east : east + fits, :]
            for q in range(fits, EAST[f]):
                for t in range(blocks):
                    at, row = (q - fits) * blocks + t, PAD + nx + q
                    X[f, row : row + 1, t * LANES : (t + 1) * LANES] = spare_recv[at : at + 1, :]
            west += WEST[f]
            east += EAST[f]
        for f in range(fields):
            got = inner_recv[step]
            X[f, :, ny:width] = jnp.where(
                top, roll(got, LANES - SLOT * (f + 1), 1), roll(got, LANES - SLOT * f, 1)
            )
            G[f] = roll(fold_recv[step], LANES - SLOT * (f + 1), 1)

    pack_rows(0, 0, FIELDS - 1)
    tile = tile_0 = send_tile(0, FIELDS)
    lead = (jnp.logical_or(far_west, first_z), far_east)
    each(*lead, lambda c: c[0].start(), tile)
    loads[5].wait()
    total = thick[0]
    for l in range(1, layers):
        total = total + thick[l]
    X[5, own, 0:ny] = (WAVE_LIMIT / layers) * total
    pack_rows(0, FIELDS - 1, FIELDS)
    pack_edges(0, FIELDS)
    each(*lead, lambda c: start_all(c[:0:-1]), tile)
    each(far_east, jnp.logical_and(far_west, jnp.logical_not(last_z)), lambda c: start_all(c[::-1]), tile)
    tile[2].start()
    start_folds(tile[3], lambda zz: zz < z)
    for _, near_copy, zz in tile[3]:
        pl.when(jnp.logical_and(top, zz == z))(near_copy.start)

    def lay_copies(step):
        def one(src, dst, zz, mm, k=0):
            leaving[k] = leaving.get(k, 0) + lines(src)
            return pltpu.make_async_remote_copy(
                src_ref=src,
                dst_ref=dst,
                send_sem=send_sem.at[k],
                recv_sem=lay_recv_sem.at[step],
                device_id={"zonal": zz, "merid": mm},
                device_id_type=MESH,
            )

        return [
            one(lay_send_r.at[step], lay_recv_w.at[step], right, m),
            one(lay_send_l.at[step], lay_recv_e.at[step], left, m),
            one(lay_pack_send.at[step, 0], lay_pack_recv.at[step, 0], z, other),
            one(lay_pack_send.at[step, 1], lay_pack_recv.at[step, 1], mirror, m, 3),
        ]

    above = lay_send_r.shape[1] // 2

    def send_layers(step, h_ref, u_ref, v_ref):
        edge = jnp.zeros((nx, LANES), jnp.float32)
        brim = jnp.zeros((nx, LANES), jnp.float32)
        for l in range(layers):
            lay_send_r[step, l : l + 1, :] = h_ref[l, nx - 1 : nx, :]
            lay_send_r[step, above + l : above + l + 1, :] = u_ref[l, nx - 1 : nx, :]
            lay_send_l[step, l : l + 1, :] = h_ref[l, 0:1, :]
            high = roll(h_ref[l, :, last:ny], l + 1, 1)
            low = roll(h_ref[l, :, 0:LANES], l, 1)
            high_v = roll(v_ref[l, :, last:ny], layers + l + 1, 1)
            edge = jnp.where(lane == l, jnp.where(bottom, high, low), edge)
            edge = jnp.where(lane == layers + l, high_v, edge)
            brim = jnp.where(lane == l, high, brim)
        lay_pack_send[step, 0] = edge
        lay_pack_send[step, 2] = brim
        for r in range(nx):
            lay_pack_send[step, 1, r : r + 1, :] = lay_pack_send[step, 2, nx - 1 - r : nx - r, :]
        return lay_copies(step)

    def start_layers(out, first):
        out[2].start()
        hold, late_fold = (late_left, mirror > z) if first else (False, False)
        pl.when(jnp.logical_and(top, jnp.logical_not(late_fold)))(out[3].start)
        pl.when(far_west)(out[0].start)
        pl.when(jnp.logical_not(hold))(out[1].start)
        pl.when(jnp.logical_not(far_west))(out[0].start)

    def wait_layers(step):
        take(lay_recv_sem.at[step], lines(lay_recv_w.at[step]) + lines(lay_recv_e.at[step]) + nx, nx)

    def wait_sent():
        drain(blank.at[0 : leaving[0]], send_sem.at[0])
        pl.when(jnp.logical_not(first_z))(lambda: drain(blank.at[0 : leaving[1]], send_sem.at[1]))
        pl.when(jnp.logical_not(first_top))(lambda: drain(blank.at[0 : leaving[5]], send_sem.at[5]))
        for k, zz in zip((4, 3, 2), mirrors):
            pl.when(jnp.logical_and(top, zz != z))(lambda k=k: drain(blank.at[0 : leaving[k]], send_sem.at[k]))

    drain(vel, load_sem.at[2])
    for load in loads[8:]:
        load.wait()
    out = send_layers(0, thick, vel_u, vel_v)

    start_layers(out, True)
    first = (z * nx - PAD).astype(jnp.float32)
    col = first + iota((rows, 1), 0).astype(jnp.float32) + float(total_x)
    far_col = float(2 * total_x - 1) - (first + iota((rows, 1), 0).astype(jnp.float32))
    spot = iota((1, width), 1)
    row = spot + m * ny
    row = jnp.where(jnp.logical_and(top, spot >= ny), row - width, row).astype(jnp.float32)
    far_row = (iota((1, LANES), 1) + (total_y - LANES)).astype(jnp.float32)
    px = jnp.zeros((rows, width), jnp.float32)
    py = jnp.zeros((rows, width), jnp.float32)
    fx = jnp.zeros((rows, LANES), jnp.float32)
    fy = jnp.zeros((rows, LANES), jnp.float32)
    for k in range(seeds.shape[1]):
        seed_x = seeds[0, k].astype(jnp.float32)
        seed_y = seeds[1, k].astype(jnp.float32)
        ca, sa = turns(seed_x, col, total_x)
        cf, sf = turns(seed_x, far_col, total_x)
        cb, sb = turns(seed_y, row, total_y)
        cg, sg = turns(seed_y, far_row, total_y)
        amp = scale[k]
        ca, sa, cf, sf = amp * ca, amp * sa, amp * cf, amp * sf
        px = px + (ca * cb - sa * sb)
        py = py + (sa * cb + ca * sb)
        fx = fx + (cf * cg - sf * sg)
        fy = fy + (sf * cg + cf * sg)
    wind_own[0] = px
    wind_own[1] = py
    wind_far[0] = fx
    wind_far[1] = fy

    layer_trial(thick, vel_u, vel_v, mid_h, mid_u, mid_v, sums, True)

    @pl.when(late_left)
    def _():
        pl.semaphore_wait(late_sem.at[0], 2)
        start_all(tile[1][-1:] + tile[1][:-1])


    @pl.when(jnp.logical_and(top, upper > 0))
    def _():
        pl.semaphore_wait(late_sem.at[1], upper)

    start_folds(tile[3], lambda zz: zz > z)
    pl.when(jnp.logical_and(top, mirror > z))(out[3].start)

    @pl.when(first_z)
    def _():
        drain(blank.at[0 : leaving[1]], send_sem.at[1])

    first_top = jnp.logical_and(first_z, top)
    pl.when(first_top)(lambda: drain(blank.at[0 : leaving[5]], send_sem.at[5]))
    pl.when(late_left)(out[1].start)

    take_tile(0, FIELDS)
    lanes = iota((rows, width), 1)
    wall = jnp.logical_and(bottom, lanes == 0)
    crown = jnp.logical_and(top, iota((rows, LANES), 1) == LANES - 1)
    far_top = iota((rows, LANES), 1) == LANES - 1

    def southern(bv, g_bv):
        return jnp.where(wall, 0.0, roll(bv, 1, 1)), roll(g_bv, 1, 1)

    for k in range(2):
        mask, far_mask = X[3 + k], G[3 + k]
        D[2 * k] = mask * X[5]
        F[2 * k] = far_mask * G[5]
        D[2 * k + 1] = mask * (STRESS_SCALE * (X[6 + k] + wind_own[k]))
        F[2 * k + 1] = far_mask * (STRESS_SCALE * (G[6 + k] + wind_far[k]))
    for k in range(2):
        D[4 + k], F[4 + k] = southern(D[2 + k], F[2 + k])

    def close_step(step, h_ref, v_ref, n_h, n_u, n_v):
        layer_edges(
            h_ref, v_ref, lay_send_r.at[step], lay_send_l.at[step], lay_recv_w.at[step], lay_recv_e.at[step],
            lay_pack_recv.at[step], n_h, n_u, n_v, mean, masks, depth, top, step == 0,
        )

    def substep(carry, masked):
        eta, bu, bv, south_v, g_eta, g_bu, g_bv, g_south_v = carry
        eta = eta - (bu - roll(bu, 1, 0) + bv - south_v)
        g_eta = g_eta - (g_bu - roll(g_bu, -1, 0) + g_bv - g_south_v)
        if masked:
            bu, bv, south_v, g_bu, g_bv, g_south_v = masked
        north, south = roll(eta, -1, 1), roll(eta, 1, 1)
        brink = jnp.where(crown, g_eta[:, LANES - 1 :], north[:, last:ny])
        north = jnp.concatenate([north[:, :last], brink, north[:, ny:]], axis=1)
        g_north = jnp.where(far_top, eta[:, ny - 1 : ny], roll(g_eta, -1, 1))
        g_south = roll(g_eta, 1, 1)
        bu = bu - D[0] * (roll(eta, -1, 0) - eta) + D[1]
        bv = bv - D[2] * (north - eta) + D[3]
        south_v = south_v - D[4] * (eta - south) + D[5]
        g_bu = g_bu - F[0] * (roll(g_eta, 1, 0) - g_eta) + F[1]
        g_bv = g_bv - F[2] * (g_north - g_eta) + F[3]
        g_south_v = g_south_v - F[4] * (g_eta - g_south) + F[5]
        mean[0] = mean[0] + bu[own, 0:ny]
        mean[1] = mean[1] + bv[own, 0:ny]
        return eta, bu, bv, south_v, g_eta, g_bu, g_bv, g_south_v

    def substeps(out, raw):
        mean[...] = jnp.zeros((2, nx, ny), jnp.float32)
        bu, bv, g_bu, g_bv = X[1], X[2], G[1], G[2]
        south_v, g_south_v = southern(bv, g_bv)
        carry = X[0], bu, bv, south_v, G[0], g_bu, g_bv, g_south_v
        masked = None
        if raw:
            bu, bv, g_bu, g_bv = X[3] * bu, X[4] * bv, G[3] * g_bu, G[4] * g_bv
            south_v, g_south_v = southern(bv, g_bv)
            masked = bu, bv, south_v, g_bu, g_bv, g_south_v
        for n in range(NSUB):
            carry = substep(carry, masked if n == 0 else None)
        for k in range(3):
            out[k, ...] = carry[k][own, 0:ny]

    masks = X[3, own, 0:ny], X[4, own, 0:ny]
    h_ref, u_ref, v_ref = thick, vel_u, vel_v
    n_h, n_u, n_v = mid_h, mid_u, mid_v
    for step in range(STEPS - 1):
        substeps(X.at[0:3, own, 0:ny], step == 0)
        pack_rows(step + 1, 0, 3)
        tile = send_tile(step + 1, 3)
        lead = (far_west, even)

        def inner_ready():
            each(*lead, lambda c: start_all(c[::-1]), tile)
            tile[2].start()

        pack_edges(step + 1, 3, inner_ready)
        start_folds(tile[3], lambda zz: zz != z)
        for _, near_copy, zz in tile[3]:
            pl.when(jnp.logical_and(top, zz == z))(near_copy.start)
        each(even, far_west, lambda c: start_all(c[::-1]), tile)
        layer_close(n_u, n_v, sums, mean, masks, depth, step == 0)
        wait_layers(step)
        close_step(step, h_ref, v_ref, n_h, n_u, n_v)
        h_ref, u_ref, v_ref = n_h, n_u, n_v
        n_h, n_u, n_v = o_h, o_u, o_v
        out = send_layers(step + 1, h_ref, u_ref, v_ref)
        start_layers(out, False)
        layer_trial(h_ref, u_ref, v_ref, n_h, n_u, n_v, sums, False)
        take_tile(step + 1, 3)
    substeps(flat, STEPS == 1)
    layer_close(n_u, n_v, sums, mean, masks, depth, False)
    wait_layers(STEPS - 1)
    close_step(STEPS - 1, h_ref, v_ref, n_h, n_u, n_v)
    wait_sent()


def body(zonal_devices, merid_devices, *args):
    thickness = args[3]
    layers, nx, ny = thickness.shape
    up = tile_up(layers)
    f32 = jnp.float32
    vmem = pl.BlockSpec(memory_space=pltpu.VMEM)
    far = pl.BlockSpec(memory_space=pltpu.HBM)
    hbm = pl.BlockSpec(memory_space=pl.ANY)
    rows = nx + 2 * PAD
    west, east = tile_up(sum(WEST)), tile_up(sum(EAST))
    spare = tile_up(sum(EAST) % 8 * ny // LANES)
    plane = jax.ShapeDtypeStruct((nx, ny), f32)
    solid = jax.ShapeDtypeStruct((layers, nx, ny), f32)
    kept = [(3, nx, ny), (layers, nx, ny), (layers, nx, ny), (layers, nx, ny)]
    room = sum(math.prod(shape) for shape in kept)
    args = list(args)
    args[7] = args[7].T
    between = pl.pallas_call(
        functools.partial(kernel, zonal_devices, merid_devices),
        out_shape=[pltpu.VMEM(shape, f32) for shape in kept],
        in_specs=[far] * 10,
        out_specs=[vmem] * len(kept),
        scratch_shapes=[
            pltpu.VMEM((layers, nx, ny), f32),
            pltpu.VMEM((2, layers, nx, ny), f32),
            pltpu.VMEM((2, nx, ny), jnp.int32),
            pltpu.SMEM(args[7].shape, jnp.int32),
            pltpu.SMEM(args[8].shape, f32),
            pltpu.VMEM((layers, nx, ny), f32),
            pltpu.VMEM((layers, nx, ny), f32),
            pltpu.VMEM((layers, nx, ny), f32),
            pltpu.VMEM((2, nx, ny), f32),
            pltpu.VMEM((4, nx, ny), f32),
            pltpu.VMEM((2, nx, ny), f32),
            pltpu.VMEM((FIELDS, rows, ny + LANES), f32),
            pltpu.VMEM((FIELDS, rows, LANES), f32),
            pltpu.VMEM((6, rows, ny + LANES), f32),
            pltpu.VMEM((6, rows, LANES), f32),
            pltpu.VMEM((2, rows, ny + LANES), f32),
            pltpu.VMEM((2, rows, LANES), f32),
            pltpu.VMEM((STEPS, west, ny), f32),
            pltpu.VMEM((STEPS, west, ny), f32),
            pltpu.VMEM((STEPS, east, ny), f32),
            pltpu.VMEM((STEPS, east, ny), f32),
            pltpu.VMEM((spare, LANES), f32),
            pltpu.VMEM((spare, LANES), f32),
            pltpu.VMEM((STEPS, 3, nx, LANES), f32),
            pltpu.VMEM((STEPS, rows, LANES), f32),
            pltpu.VMEM((STEPS, rows, LANES), f32),
            pltpu.VMEM((STEPS, 2 * up, ny), f32),
            pltpu.VMEM((STEPS, up, ny), f32),
            pltpu.VMEM((STEPS, 2 * up, ny), f32),
            pltpu.VMEM((STEPS, up, ny), f32),
            pltpu.VMEM((STEPS, 3, nx, LANES), f32),
            pltpu.VMEM((STEPS, 2, nx, LANES), f32),
            pltpu.VMEM((4 * (west + east) * ny // LANES, LANES), f32),
            pltpu.SemaphoreType.DMA((5,)),
            pltpu.SemaphoreType.DMA((6,)),
            pltpu.SemaphoreType.DMA((STEPS,)),
            pltpu.SemaphoreType.DMA((STEPS,)),
            pltpu.SemaphoreType.REGULAR((2,)),
        ],
        compiler_params=pltpu.CompilerParams(
            collective_id=0, has_side_effects=True, vmem_limit_bytes=VMEM_BYTES - 4 * room - SPARE
        ),
        name="ocean",
    )(*args)
    return pl.pallas_call(
        last_kernel,
        out_shape=(plane, plane, plane, solid, solid, solid),
        in_specs=[vmem] * len(kept),
        out_specs=[hbm] * 6,
        scratch_shapes=[pltpu.SemaphoreType.DMA((4,))],
        compiler_params=pltpu.CompilerParams(vmem_limit_bytes=24 * 1024 * 1024),
        name="last",
    )(*between)


def solution(mesh):
    field = P(("members", "zonal"), "merid")
    solid = P(None, ("members", "zonal"), "merid")
    fixed = P(None, "zonal", "merid")
    return jax.shard_map(
        functools.partial(body, mesh.shape["zonal"], mesh.shape["merid"]),
        mesh=mesh,
        in_specs=(
            field, field, field, solid, solid, solid, fixed, P("members", None), P("members"), fixed,
        ),
        out_specs=(field, field, field, solid, solid, solid),
        check_vma=False,
    )
```

```python
import functools
import math

import jax
import jax.numpy as jnp
from jax import lax
from jax.experimental import pallas as pl
from jax.experimental.pallas import tpu as pltpu
from jax.sharding import PartitionSpec as P

NSUB = 6
STEPS = 2
MARGIN = NSUB
PAD = 8

WAVE_LIMIT = 0.225
STRESS_SCALE = 0.1
FLUX_STEP = 0.05
PRESS_COEF = 0.05
LANES = 128
VMEM_BYTES = 67043328
SPARE = 1 << 15
FIELDS = 8
SLOT = LANES // FIELDS
WEST = (NSUB - 1, NSUB, NSUB - 1, NSUB - 1, NSUB - 2, NSUB - 1, NSUB - 1, NSUB - 2)
EAST = (NSUB, NSUB, NSUB) + (NSUB - 1,) * 5
ORDER = (0, 1, 2, 3, 4, 6, 7, 5)
CUT = 24
MESH = pl.DeviceIdType.MESH


def roll(value, shift, axis):
    return pltpu.roll(value, shift % value.shape[axis], axis)


def iota(shape, axis):
    return lax.broadcasted_iota(jnp.int32, shape, axis)


def turns(seed, index, total):
    part = seed * index * (1.0 / total)
    angle = (2.0 * math.pi) * (part - jnp.floor(part))
    return jnp.cos(angle), jnp.sin(angle)


def lines(ref):
    return math.prod(ref.shape) // LANES


def drain(ref, sem):
    pltpu.make_async_copy(ref, ref, sem).wait()


def tile_up(count):
    return -(-count // 8) * 8


def layer_trial(h_ref, u_ref, v_ref, o_h, o_u, o_v, sums, deep):
    layers, nx, ny = h_ref.shape
    at_east = iota((nx, ny), 0) == nx - 1
    at_north = iota((nx, ny), 1) == ny - 1
    zero = jnp.zeros((nx, ny), jnp.float32)
    press_u, press_v, sum_u, sum_v = zero, zero, zero, zero
    deep_u, deep_v = zero, zero
    for l in range(layers):
        h, u, v = h_ref[l], u_ref[l], v_ref[l]
        h_east, h_north = roll(h, -1, 0), roll(h, -1, 1)
        hu = (h + h_east) * 0.5
        hv = (h + h_north) * 0.5
        if deep:
            deep_u = deep_u + hu
            deep_v = deep_v + hv
        flux_u = jnp.where(at_east, 0.0, u * hu)
        flux_v = jnp.where(at_north, 0.0, v * hv)
        press_u = press_u + (h_east - h)
        press_v = press_v + (h_north - h)
        trial_u = u - PRESS_COEF * press_u
        trial_v = v - PRESS_COEF * press_v
        sum_u = sum_u + hu * trial_u
        sum_v = sum_v + hv * trial_v
        o_u[l] = trial_u
        o_v[l] = trial_v
        o_h[l] = h - FLUX_STEP * (flux_u - roll(flux_u, 1, 0) + flux_v - roll(flux_v, 1, 1))
    sums[0] = sum_u
    sums[1] = sum_v
    if deep:
        sums[2] = deep_u
        sums[3] = deep_v


def layer_close(o_u, o_v, sums, mean, masks, depth, deep):
    if deep:
        depth[0] = 1.0 / sums[2]
        depth[1] = 1.0 / sums[3]
    for k, out in enumerate((o_u, o_v)):
        fix = (mean[k] * (1.0 / NSUB) - sums[k]) * depth[k]
        mask = masks[k]
        for l in range(out.shape[0]):
            out[l] = mask * (out[l] + fix)


def layer_edges(h_ref, v_ref, own_r, own_l, recv_w, recv_e, packs, o_h, o_u, o_v, mean, masks, depth, top, deep):
    layers, nx, ny = h_ref.shape
    up = own_l.shape[0]
    layer = iota((up, ny), 0)
    h_last, u_last, h_first = own_r[0:up], own_r[up:], own_l[...]
    h_e, h_w, u_w = recv_e[...], recv_w[0:up], recv_w[up:]
    hu = (h_last + h_e) * 0.5
    press = h_e - h_last
    step = 1
    while step < layers:
        press = press + jnp.where(layer >= step, roll(press, step, 0), 0.0)
        step *= 2
    trial = u_last - PRESS_COEF * press
    outflow = FLUX_STEP * (u_last * hu)
    inflow = FLUX_STEP * (u_w * ((h_w + h_first) * 0.5))
    whole = lambda a: jnp.sum(jnp.where(layer < layers, a, 0.0), axis=0, keepdims=True)
    if deep:
        depth[0, nx - 1 : nx, :] = 1.0 / whole(hu)
    fix = (mean[0, nx - 1 : nx, :] * (1.0 / NSUB) - whole(hu * trial)) * depth[0, nx - 1 : nx, :]
    edge_u = masks[0][nx - 1 : nx, :] * (trial + fix)
    for l in range(layers):
        o_u[l, nx - 1 : nx, :] = edge_u[l : l + 1]
        o_h[l, nx - 1 : nx, :] = o_h[l, nx - 1 : nx, :] - outflow[l : l + 1]
        o_h[l, 0:1, :] = o_h[l, 0:1, :] + inflow[l : l + 1]

    lane = iota((nx, LANES), 1)
    last = ny - LANES
    at_end = lane == LANES - 1
    at_start = jnp.logical_and(top, lane == 0)
    side = packs[0]
    cap = jnp.where(top, packs[1], side)
    press, total, deep_v = 0.0, 0.0, 0.0
    trials = []
    for l in range(layers):
        h, v = h_ref[l, :, last:ny], v_ref[l, :, last:ny]
        h_north = roll(cap, LANES - 1 - l, 1)
        hv = (h + h_north) * 0.5
        press = press + (h_north - h)
        trials.append(v - PRESS_COEF * press)
        total = total + hv * trials[l]
        deep_v = deep_v + hv
        o_h[l, :, last:ny] = o_h[l, :, last:ny] - jnp.where(at_end, FLUX_STEP * (v * hv), 0.0)
        h_south, v_south = roll(side, -l, 1), roll(side, -(layers + l), 1)
        inflow = FLUX_STEP * (v_south * ((h_south + h_ref[l, :, 0:LANES]) * 0.5))
        o_h[l, :, 0:LANES] = o_h[l, :, 0:LANES] + jnp.where(at_start, inflow, 0.0)
    if deep:
        depth[1, :, last:ny] = jnp.where(at_end, 1.0 / deep_v, depth[1, :, last:ny])
    fix = (mean[1, :, last:ny] * (1.0 / NSUB) - total) * depth[1, :, last:ny]
    for l in range(layers):
        edge_v = masks[1][:, last:ny] * (trials[l] + fix)
        o_v[l, :, last:ny] = jnp.where(at_end, edge_v, o_v[l, :, last:ny])


def last_kernel(flat, n_h, n_u, n_v, o_eta, o_bu, o_bv, o_h, o_u, o_v, sems):
    moves = [(flat.at[k], o, 0) for k, o in enumerate((o_eta, o_bu, o_bv))]
    moves += [(n_h, o_h, 1), (n_u, o_u, 2), (n_v, o_v, 3)]
    copies = [pltpu.make_async_copy(src, dst, sems.at[k]) for src, dst, k in moves]
    for copy in copies:
        copy.start()
    drain(flat, sems.at[0])
    for copy in copies[3:]:
        copy.wait()


def kernel(
    zonal_devices,
    merid_devices,
    height_any,
    trans_u_any,
    trans_v_any,
    thick_any,
    vel_u_any,
    vel_v_any,
    faces_any,
    seeds_any,
    scale_any,
    base_any,
    flat,
    o_h,
    o_u,
    o_v,
    thick,
    vel,
    faces,
    seeds,
    scale,
    mid_h,
    mid_u,
    mid_v,
    mean,
    sums,
    depth,
    X,
    G,
    D,
    F,
    wind_own,
    wind_far,
    west_send,
    west_recv,
    east_send,
    east_recv,
    spare_send,
    spare_recv,
    pack_send,
    inner_recv,
    fold_recv,
    lay_send_r,
    lay_send_l,
    lay_recv_w,
    lay_recv_e,
    lay_pack_send,
    lay_pack_recv,
    blank,
    load_sem,
    send_sem,
    recv_sem,
    lay_recv_sem,
    late_sem,
):
    layers, nx, ny = thick.shape
    Z = zonal_devices
    total_x, total_y = nx * Z, ny * merid_devices
    z = lax.axis_index("zonal")
    m = lax.axis_index("merid")
    other = 1 - m
    bottom = m == 0
    top = m == merid_devices - 1
    right, left = lax.rem(z + 1, Z), lax.rem(z + Z - 1, Z)
    mirror = Z - 1 - z
    mirror_e, mirror_w = lax.rem(mirror + 1, Z), lax.rem(mirror + Z - 1, Z)
    rows = nx + 2 * PAD
    width = ny + LANES
    last = ny - LANES
    own = slice(PAD, PAD + nx)
    lane = iota((nx, LANES), 1)

    barrier = pltpu.get_barrier_semaphore()
    first_z, last_z = z == 0, z == Z - 1
    late_left = jnp.logical_or(first_z, last_z)
    mirrors = (mirror_w, mirror, mirror_e)

    def greet(sem, zz, mm):
        pl.semaphore_signal(sem, inc=1, device_id={"zonal": zz, "merid": mm}, device_id_type=MESH)

    greet(barrier, z, other)
    for mm in (m, other):
        greet(barrier, left, mm)
        pl.when(z < Z - 2)(lambda mm=mm: greet(barrier, right, mm))

    for zz in mirrors:

        @pl.when(jnp.logical_and(top, zz > z))
        def _():
            greet(barrier, zz, m)

    moves = (
        (faces_any, faces),
        (height_any, X.at[0, own, 0:ny]),
        (trans_u_any, X.at[1, own, 0:ny]),
        (trans_v_any, X.at[2, own, 0:ny]),
        (base_any, X.at[6:8, own, 0:ny]),
        (thick_any, thick),
        (vel_u_any, vel.at[0]),
        (vel_v_any, vel.at[1]),
        (seeds_any, seeds),
        (scale_any, scale),
    )
    group = (0, 0, 0, 0, 0, 1, 2, 2, 3, 4)
    vel_u, vel_v = vel.at[0], vel.at[1]
    loads = [pltpu.make_async_copy(src, dst, load_sem.at[k]) for k, (src, dst) in zip(group, moves)]
    for load in loads:
        load.start()

    near = 3 + jnp.where(jnp.logical_or(first_z, last_z), 0, 2)
    lower = sum((zz < z).astype(jnp.int32) for zz in mirrors)
    upper = sum((zz > z).astype(jnp.int32) for zz in mirrors)
    pl.semaphore_wait(barrier, near + jnp.where(top, lower, 0))

    @pl.when(z >= Z - 2)
    def _():
        for mm in (m, other):
            greet(late_sem.at[0], right, mm)

    for zz in mirrors:

        @pl.when(jnp.logical_and(top, zz < z))
        def _():
            greet(late_sem.at[1], zz, m)

    drain(blank.at[0 : sum(lines(dst) for _, dst in moves[:5])], load_sem.at[0])
    X[3, own, 0:ny] = faces[0].astype(jnp.float32)
    X[4, own, 0:ny] = faces[1].astype(jnp.float32)

    blocks = ny // LANES
    full_east = sum(EAST) // 8 * 8

    def pack_rows(step, start, stop):
        west = sum(WEST[f] for f in ORDER[:start])
        east = sum(EAST[f] for f in ORDER[:start])
        for f in ORDER[start:stop]:
            west_send[step, west : west + WEST[f], :] = X[f, PAD + nx - WEST[f] : PAD + nx, 0:ny]
            fits = EAST[f] if step else min(EAST[f], full_east - east)
            east_send[step, east : east + fits, :] = X[f, PAD : PAD + fits, 0:ny]
            for q in range(fits, EAST[f]):
                for t in range(blocks):
                    at = (q - fits) * blocks + t
                    spare_send[at : at + 1, :] = X[f, PAD + q : PAD + q + 1, t * LANES : (t + 1) * LANES]
            west += WEST[f]
            east += EAST[f]

    def pack_edges(step, fields, between=lambda: None):
        inner = jnp.zeros((nx, LANES), jnp.float32)
        crest = jnp.zeros((nx, LANES), jnp.float32)
        for f in range(fields):
            here = jnp.logical_and(lane >= f * SLOT, lane < (f + 1) * SLOT)
            high = roll(X[f, own, last:ny], SLOT * (f + 1), 1)
            low = roll(X[f, own, 0:LANES], SLOT * f, 1)
            crest = jnp.where(here, high, crest)
            inner = jnp.where(here, jnp.where(bottom, high, low), inner)
        pack_send[step, 0] = inner
        between()
        pack_send[step, 2] = crest
        for r in range(nx):
            pack_send[step, 1, r : r + 1, :] = pack_send[step, 2, nx - 1 - r : nx - r, :]

    leaving = {}

    def send_tile(step, fields):
        def send(src, dst, k, zz, mm):
            leaving[k] = leaving.get(k, 0) + lines(src)
            return pltpu.make_async_remote_copy(
                src_ref=src,
                dst_ref=dst,
                send_sem=send_sem.at[k],
                recv_sem=recv_sem.at[step],
                device_id={"zonal": zz, "merid": mm},
                device_id_type=MESH,
            )

        def rows_of(src, dst, k, zz, count):
            cuts = [0, CUT, count] if count > CUT else [0, count]
            parts = [slice(low, high) for low, high in zip(cuts[:-1], cuts[1:])]
            return [send(src.at[step, p], dst.at[step, p], 5 * k if n else k, zz, m) for n, p in enumerate(parts)]

        tail, whole, start = slice(nx - PAD, nx), slice(0, nx), slice(0, PAD)
        places = (slice(0, PAD), own, slice(PAD + nx, rows))
        inner = lambda s, part: (pack_send.at[step, 0, part], inner_recv.at[step, places[s]])
        west = rows_of(west_send, west_recv, 0, right, tile_up(sum(WEST[:fields])))
        east = rows_of(east_send, east_recv, int(step == 0), left, tile_up(sum(EAST[:fields])) if step else full_east)
        if not step:
            east.append(send(spare_send, spare_recv, 5, left, m))
        west.append(send(*inner(0, tail), 0, right, other))
        east.append(send(*inner(2, start), 0 if step else 5, left, other))
        across = send(*inner(1, whole), 0, z, other)
        folds = []
        for s, part, zz in ((2, start, mirror_w), (1, whole, mirror), (0, tail, mirror_e)):
            src, dst = pack_send.at[step, 1, part], fold_recv.at[step, places[s]]
            near = pltpu.make_async_copy(src, dst, recv_sem.at[step])
            folds.append((send(src, dst, 2 + s, zz, m), near, zz))
        return west, east, across, folds

    even = lax.rem(z, 2) == 0

    def start_all(copies):
        for copy in copies:
            copy.start()

    far_west, far_east = jnp.logical_not(even), jnp.logical_and(even, jnp.logical_not(first_z))

    def each(west_when, east_when, act, tile):
        pl.when(west_when)(lambda: act(tile[0]))
        pl.when(east_when)(lambda: act(tile[1]))

    def start_folds(folds, chosen):
        for far_copy, _, zz in folds:
            pl.when(jnp.logical_and(top, chosen(zz)))(far_copy.start)

    def take(sem, always, at_top):
        pl.when(bottom)(lambda: drain(blank.at[0:always], sem))
        pl.when(top)(lambda: drain(blank.at[0 : always + at_top], sem))

    def take_tile(step, fields):
        count = tile_up(sum(WEST[:fields])) + (tile_up(sum(EAST[:fields])) if step else full_east)
        take(recv_sem.at[step], count * blocks + rows + (0 if step else lines(spare_recv)), rows)

        west = east = 0
        for f in ORDER[:fields]:
            X[f, PAD - WEST[f] : PAD, 0:ny] = west_recv[step, west : west + WEST[f], :]
            fits = EAST[f] if step else min(EAST[f], full_east - east)
            X[f, PAD + nx : PAD + nx + fits, 0:ny] = east_recv[step, east : east + fits, :]
            for q in range(fits, EAST[f]):
                for t in range(blocks):
                    at, row = (q - fits) * blocks + t, PAD + nx + q
                    X[f, row : row + 1, t * LANES : (t + 1) * LANES] = spare_recv[at : at + 1, :]
            west += WEST[f]
            east += EAST[f]
        for f in range(fields):
            got = inner_recv[step]
            X[f, :, ny:width] = jnp.where(
                top, roll(got, LANES - SLOT * (f + 1), 1), roll(got, LANES - SLOT * f, 1)
            )
            G[f] = roll(fold_recv[step], LANES - SLOT * (f + 1), 1)

    pack_rows(0, 0, FIELDS - 1)
    tile = tile_0 = send_tile(0, FIELDS)
    lead = (jnp.logical_or(far_west, first_z), far_east)
    each(*lead, lambda c: c[0].start(), tile)
    loads[5].wait()
    total = thick[0]
    for l in range(1, layers):
        total = total + thick[l]
    X[5, own, 0:ny] = (WAVE_LIMIT / layers) * total
    pack_rows(0, FIELDS - 1, FIELDS)
    pack_edges(0, FIELDS)
    each(*lead, lambda c: start_all(c[:0:-1]), tile)
    each(far_east, jnp.logical_and(far_west, jnp.logical_not(last_z)), lambda c: start_all(c[::-1]), tile)
    tile[2].start()
    start_folds(tile[3], lambda zz: zz < z)
    for _, near_copy, zz in tile[3]:
        pl.when(jnp.logical_and(top, zz == z))(near_copy.start)

    def lay_copies(step):
        def one(src, dst, zz, mm, k=0):
            leaving[k] = leaving.get(k, 0) + lines(src)
            return pltpu.make_async_remote_copy(
                src_ref=src,
                dst_ref=dst,
                send_sem=send_sem.at[k],
                recv_sem=lay_recv_sem.at[step],
                device_id={"zonal": zz, "merid": mm},
                device_id_type=MESH,
            )

        return [
            one(lay_send_r.at[step], lay_recv_w.at[step], right, m),
            one(lay_send_l.at[step], lay_recv_e.at[step], left, m),
            one(lay_pack_send.at[step, 0], lay_pack_recv.at[step, 0], z, other),
            one(lay_pack_send.at[step, 1], lay_pack_recv.at[step, 1], mirror, m, 3),
        ]

    above = lay_send_r.shape[1] // 2

    def send_layers(step, h_ref, u_ref, v_ref):
        edge = jnp.zeros((nx, LANES), jnp.float32)
        brim = jnp.zeros((nx, LANES), jnp.float32)
        for l in range(layers):
            lay_send_r[step, l : l + 1, :] = h_ref[l, nx - 1 : nx, :]
            lay_send_r[step, above + l : above + l + 1, :] = u_ref[l, nx - 1 : nx, :]
            lay_send_l[step, l : l + 1, :] = h_ref[l, 0:1, :]
            high = roll(h_ref[l, :, last:ny], l + 1, 1)
            low = roll(h_ref[l, :, 0:LANES], l, 1)
            high_v = roll(v_ref[l, :, last:ny], layers + l + 1, 1)
            edge = jnp.where(lane == l, jnp.where(bottom, high, low), edge)
            edge = jnp.where(lane == layers + l, high_v, edge)
            brim = jnp.where(lane == l, high, brim)
        lay_pack_send[step, 0] = edge
        lay_pack_send[step, 2] = brim
        for r in range(nx):
            lay_pack_send[step, 1, r : r + 1, :] = lay_pack_send[step, 2, nx - 1 - r : nx - r, :]
        return lay_copies(step)

    def start_layers(out, first):
        out[2].start()
        hold, late_fold = (late_left, mirror > z) if first else (False, False)
        pl.when(jnp.logical_and(top, jnp.logical_not(late_fold)))(out[3].start)
        pl.when(far_west)(out[0].start)
        pl.when(jnp.logical_not(hold))(out[1].start)
        pl.when(jnp.logical_not(far_west))(out[0].start)

    def wait_layers(step):
        take(lay_recv_sem.at[step], lines(lay_recv_w.at[step]) + lines(lay_recv_e.at[step]) + nx, nx)

    def wait_sent():
        drain(blank.at[0 : leaving[0]], send_sem.at[0])
        pl.when(jnp.logical_not(first_z))(lambda: drain(blank.at[0 : leaving[1]], send_sem.at[1]))
        pl.when(jnp.logical_not(first_top))(lambda: drain(blank.at[0 : leaving[5]], send_sem.at[5]))
        for k, zz in zip((4, 3, 2), mirrors):
            pl.when(jnp.logical_and(top, zz != z))(lambda k=k: drain(blank.at[0 : leaving[k]], send_sem.at[k]))

    drain(vel, load_sem.at[2])
    for load in loads[8:]:
        load.wait()
    out = send_layers(0, thick, vel_u, vel_v)

    start_layers(out, True)
    first = (z * nx - PAD).astype(jnp.float32)
    col = first + iota((rows, 1), 0).astype(jnp.float32) + float(total_x)
    far_col = float(2 * total_x - 1) - (first + iota((rows, 1), 0).astype(jnp.float32))
    spot = iota((1, width), 1)
    row = spot + m * ny
    row = jnp.where(jnp.logical_and(top, spot >= ny), row - width, row).astype(jnp.float32)
    far_row = (iota((1, LANES), 1) + (total_y - LANES)).astype(jnp.float32)
    px = jnp.zeros((rows, width), jnp.float32)
    py = jnp.zeros((rows, width), jnp.float32)
    fx = jnp.zeros((rows, LANES), jnp.float32)
    fy = jnp.zeros((rows, LANES), jnp.float32)
    for k in range(seeds.shape[1]):
        seed_x = seeds[0, k].astype(jnp.float32)
        seed_y = seeds[1, k].astype(jnp.float32)
        ca, sa = turns(seed_x, col, total_x)
        cf, sf = turns(seed_x, far_col, total_x)
        cb, sb = turns(seed_y, row, total_y)
        cg, sg = turns(seed_y, far_row, total_y)
        amp = scale[k]
        ca, sa, cf, sf = amp * ca, amp * sa, amp * cf, amp * sf
        px = px + (ca * cb - sa * sb)
        py = py + (sa * cb + ca * sb)
        fx = fx + (cf * cg - sf * sg)
        fy = fy + (sf * cg + cf * sg)
    wind_own[0] = px
    wind_own[1] = py
    wind_far[0] = fx
    wind_far[1] = fy

    layer_trial(thick, vel_u, vel_v, mid_h, mid_u, mid_v, sums, True)

    @pl.when(late_left)
    def _():
        pl.semaphore_wait(late_sem.at[0], 2)
        start_all(tile[1][-1:] + tile[1][:-1])


    @pl.when(jnp.logical_and(top, upper > 0))
    def _():
        pl.semaphore_wait(late_sem.at[1], upper)

    start_folds(tile[3], lambda zz: zz > z)
    pl.when(jnp.logical_and(top, mirror > z))(out[3].start)

    @pl.when(first_z)
    def _():
        drain(blank.at[0 : leaving[1]], send_sem.at[1])

    first_top = jnp.logical_and(first_z, top)
    pl.when(first_top)(lambda: drain(blank.at[0 : leaving[5]], send_sem.at[5]))
    pl.when(late_left)(out[1].start)

    take_tile(0, FIELDS)
    lanes = iota((rows, width), 1)
    wall = jnp.logical_and(bottom, lanes == 0)
    crown = jnp.logical_and(top, iota((rows, LANES), 1) == LANES - 1)
    far_top = iota((rows, LANES), 1) == LANES - 1

    def southern(bv, g_bv):
        return jnp.where(wall, 0.0, roll(bv, 1, 1)), roll(g_bv, 1, 1)

    for k in range(2):
        mask, far_mask = X[3 + k], G[3 + k]
        D[2 * k] = mask * X[5]
        F[2 * k] = far_mask * G[5]
        D[2 * k + 1] = mask * (STRESS_SCALE * (X[6 + k] + wind_own[k]))
        F[2 * k + 1] = far_mask * (STRESS_SCALE * (G[6 + k] + wind_far[k]))
    for k in range(2):
        D[4 + k], F[4 + k] = southern(D[2 + k], F[2 + k])

    def close_step(step, h_ref, v_ref, n_h, n_u, n_v):
        layer_edges(
            h_ref, v_ref, lay_send_r.at[step], lay_send_l.at[step], lay_recv_w.at[step], lay_recv_e.at[step],
            lay_pack_recv.at[step], n_h, n_u, n_v, mean, masks, depth, top, step == 0,
        )

    def substep(carry, masked):
        eta, bu, bv, south_v, g_eta, g_bu, g_bv, g_south_v = carry
        eta = eta - (bu - roll(bu, 1, 0) + bv - south_v)
        g_eta = g_eta - (g_bu - roll(g_bu, -1, 0) + g_bv - g_south_v)
        if masked:
            bu, bv, south_v, g_bu, g_bv, g_south_v = masked
        north, south = roll(eta, -1, 1), roll(eta, 1, 1)
        brink = jnp.where(crown, g_eta[:, LANES - 1 :], north[:, last:ny])
        north = jnp.concatenate([north[:, :last], brink, north[:, ny:]], axis=1)
        g_north = jnp.where(far_top, eta[:, ny - 1 : ny], roll(g_eta, -1, 1))
        g_south = roll(g_eta, 1, 1)
        bu = bu - D[0] * (roll(eta, -1, 0) - eta) + D[1]
        bv = bv - D[2] * (north - eta) + D[3]
        south_v = south_v - D[4] * (eta - south) + D[5]
        g_bu = g_bu - F[0] * (roll(g_eta, 1, 0) - g_eta) + F[1]
        g_bv = g_bv - F[2] * (g_north - g_eta) + F[3]
        g_south_v = g_south_v - F[4] * (g_eta - g_south) + F[5]
        mean[0] = mean[0] + bu[own, 0:ny]
        mean[1] = mean[1] + bv[own, 0:ny]
        return eta, bu, bv, south_v, g_eta, g_bu, g_bv, g_south_v

    def substeps(out, raw):
        mean[...] = jnp.zeros((2, nx, ny), jnp.float32)
        bu, bv, g_bu, g_bv = X[1], X[2], G[1], G[2]
        south_v, g_south_v = southern(bv, g_bv)
        carry = X[0], bu, bv, south_v, G[0], g_bu, g_bv, g_south_v
        masked = None
        if raw:
            bu, bv, g_bu, g_bv = X[3] * bu, X[4] * bv, G[3] * g_bu, G[4] * g_bv
            south_v, g_south_v = southern(bv, g_bv)
            masked = bu, bv, south_v, g_bu, g_bv, g_south_v
        for n in range(NSUB):
            carry = substep(carry, masked if n == 0 else None)
        for k in range(3):
            out[k, ...] = carry[k][own, 0:ny]

    masks = X[3, own, 0:ny], X[4, own, 0:ny]
    h_ref, u_ref, v_ref = thick, vel_u, vel_v
    n_h, n_u, n_v = mid_h, mid_u, mid_v
    for step in range(STEPS - 1):
        substeps(X.at[0:3, own, 0:ny], step == 0)
        pack_rows(step + 1, 0, 3)
        tile = send_tile(step + 1, 3)
        lead = (far_west, even)

        def inner_ready():
            each(*lead, lambda c: start_all(c[::-1]), tile)
            tile[2].start()

        pack_edges(step + 1, 3, inner_ready)
        start_folds(tile[3], lambda zz: zz != z)
        for _, near_copy, zz in tile[3]:
            pl.when(jnp.logical_and(top, zz == z))(near_copy.start)
        each(even, far_west, lambda c: start_all(c[::-1]), tile)
        layer_close(n_u, n_v, sums, mean, masks, depth, step == 0)
        wait_layers(step)
        close_step(step, h_ref, v_ref, n_h, n_u, n_v)
        h_ref, u_ref, v_ref = n_h, n_u, n_v
        n_h, n_u, n_v = o_h, o_u, o_v
        out = send_layers(step + 1, h_ref, u_ref, v_ref)
        start_layers(out, False)
        layer_trial(h_ref, u_ref, v_ref, n_h, n_u, n_v, sums, False)
        take_tile(step + 1, 3)
    substeps(flat, STEPS == 1)
    layer_close(n_u, n_v, sums, mean, masks, depth, False)
    wait_layers(STEPS - 1)
    close_step(STEPS - 1, h_ref, v_ref, n_h, n_u, n_v)
    wait_sent()


def body(zonal_devices, merid_devices, *args):
    thickness = args[3]
    layers, nx, ny = thickness.shape
    up = tile_up(layers)
    f32 = jnp.float32
    vmem = pl.BlockSpec(memory_space=pltpu.VMEM)
    far = pl.BlockSpec(memory_space=pltpu.HBM)
    hbm = pl.BlockSpec(memory_space=pl.ANY)
    rows = nx + 2 * PAD
    west, east = tile_up(sum(WEST)), tile_up(sum(EAST))
    spare = tile_up(sum(EAST) % 8 * ny // LANES)
    plane = jax.ShapeDtypeStruct((nx, ny), f32)
    solid = jax.ShapeDtypeStruct((layers, nx, ny), f32)
    kept = [(3, nx, ny), (layers, nx, ny), (layers, nx, ny), (layers, nx, ny)]
    room = sum(math.prod(shape) for shape in kept)
    args = list(args)
    args[7] = args[7].T
    between = pl.pallas_call(
        functools.partial(kernel, zonal_devices, merid_devices),
        out_shape=[pltpu.VMEM(shape, f32) for shape in kept],
        in_specs=[far] * 10,
        out_specs=[vmem] * len(kept),
        scratch_shapes=[
            pltpu.VMEM((layers, nx, ny), f32),
            pltpu.VMEM((2, layers, nx, ny), f32),
            pltpu.VMEM((2, nx, ny), jnp.int32),
            pltpu.SMEM(args[7].shape, jnp.int32),
            pltpu.SMEM(args[8].shape, f32),
            pltpu.VMEM((layers, nx, ny), f32),
            pltpu.VMEM((layers, nx, ny), f32),
            pltpu.VMEM((layers, nx, ny), f32),
            pltpu.VMEM((2, nx, ny), f32),
            pltpu.VMEM((4, nx, ny), f32),
            pltpu.VMEM((2, nx, ny), f32),
            pltpu.VMEM((FIELDS, rows, ny + LANES), f32),
            pltpu.VMEM((FIELDS, rows, LANES), f32),
            pltpu.VMEM((6, rows, ny + LANES), f32),
            pltpu.VMEM((6, rows, LANES), f32),
            pltpu.VMEM((2, rows, ny + LANES), f32),
            pltpu.VMEM((2, rows, LANES), f32),
            pltpu.VMEM((STEPS, west, ny), f32),
            pltpu.VMEM((STEPS, west, ny), f32),
            pltpu.VMEM((STEPS, east, ny), f32),
            pltpu.VMEM((STEPS, east, ny), f32),
            pltpu.VMEM((spare, LANES), f32),
            pltpu.VMEM((spare, LANES), f32),
            pltpu.VMEM((STEPS, 3, nx, LANES), f32),
            pltpu.VMEM((STEPS, rows, LANES), f32),
            pltpu.VMEM((STEPS, rows, LANES), f32),
            pltpu.VMEM((STEPS, 2 * up, ny), f32),
            pltpu.VMEM((STEPS, up, ny), f32),
            pltpu.VMEM((STEPS, 2 * up, ny), f32),
            pltpu.VMEM((STEPS, up, ny), f32),
            pltpu.VMEM((STEPS, 3, nx, LANES), f32),
            pltpu.VMEM((STEPS, 2, nx, LANES), f32),
            pltpu.VMEM((4 * (west + east) * ny // LANES, LANES), f32),
            pltpu.SemaphoreType.DMA((5,)),
            pltpu.SemaphoreType.DMA((6,)),
            pltpu.SemaphoreType.DMA((STEPS,)),
            pltpu.SemaphoreType.DMA((STEPS,)),
            pltpu.SemaphoreType.REGULAR((2,)),
        ],
        compiler_params=pltpu.CompilerParams(
            collective_id=0, has_side_effects=True, vmem_limit_bytes=VMEM_BYTES - 4 * room - SPARE
        ),
        name="ocean",
    )(*args)
    return pl.pallas_call(
        last_kernel,
        out_shape=(plane, plane, plane, solid, solid, solid),
        in_specs=[vmem] * len(kept),
        out_specs=[hbm] * 6,
        scratch_shapes=[pltpu.SemaphoreType.DMA((4,))],
        compiler_params=pltpu.CompilerParams(vmem_limit_bytes=24 * 1024 * 1024),
        name="last",
    )(*between)


def solution(mesh):
    field = P(("members", "zonal"), "merid")
    solid = P(None, ("members", "zonal"), "merid")
    fixed = P(None, "zonal", "merid")
    return jax.shard_map(
        functools.partial(body, mesh.shape["zonal"], mesh.shape["merid"]),
        mesh=mesh,
        in_specs=(
            field, field, field, solid, solid, solid, fixed, P("members", None), P("members"), fixed,
        ),
        out_specs=(field, field, field, solid, solid, solid),
        check_vma=False,
    )
```
